32 devices in a mesh: dp: 4 (over y, z), pp: 8 (over x, core).
Axes of the slice: x: 4, y: 2, z: 2, core: 2. Of those that a mesh axis runs over, the one named last changes fastest.
The devices are a block of a 4x4x8 slice.
Arguments:
- x_in: bfloat16 [4, 16, 128, 1536], P('dp'), parts along dimension 0
- cond_vec: bfloat16 [4, 1536], P('dp'), parts along dimension 0
- pos_ids: int32 [16, 128, 3], replicated
- w_mod: bfloat16 [8, 1536, 4608], P('pp')
- b_mod: bfloat16 [8, 4608], P('pp')
- w_one: bfloat16 [8, 1536, 10752], P('pp')
- b_one: bfloat16 [8, 10752], P('pp')
- qk_scale: bfloat16 [8, 2, 64], P('pp')
- w_two: bfloat16 [8, 7680, 1536], P('pp')
- b_two: bfloat16 [8, 1536], P('pp')
- k_prev: bfloat16 [8, 4, 16, 128, 1536], P('pp', 'dp'), parts along dimension 1
- v_prev: bfloat16 [8, 4, 16, 128, 1536], P('pp', 'dp'), parts along dimension 1
Outputs:
- output 1: bfloat16 [4, 16, 128, 1536], P('dp', 'pp'), parts along dimension 0
- output 2: bfloat16 [8, 4, 16, 128, 1536], P('pp', 'dp'), parts along dimension 1
- output 3: bfloat16 [8, 4, 16, 128, 1536], P('pp', 'dp'), parts along dimension 1
There are 4 independent parts. The reference program is written for one: setup_inputs(seed, part) draws one part's arguments, and reference() takes and returns one part's arrays. A program takes and returns all parts, laid end to end along the dimension named above; an argument that names none is the same for every part.
All inputs are finite; a program needn't handle non-finite values.
Results may differ from the reference program's by a relative error of at most 0.0148771.
Values are sent between devices in bfloat16 or wider.
A program may use at most 768 MiB of HBM per device.

```python
import math
import jax
import jax.numpy as jnp
from jax import lax

WIDTH = 1536
HEAD_DIM = 64
MLP_DIM = 6144
BATCH = 1
PATCHES = 16
PATCH_TOK = 128
LAYERS = 8
GRID_W = 64

SEQ = PATCHES * PATCH_TOK
QK_GAIN = math.log(SEQ / 16) ** 0.25


def make_ids(key):
    id_keys = jax.random.split(key, 3)
    frame_idx = jax.random.randint(id_keys[0], (), 0, 8, dtype=jnp.int32)
    row_off = jax.random.randint(id_keys[1], (), 0, 64, dtype=jnp.int32)
    col_off = jax.random.randint(id_keys[2], (), 0, 64, dtype=jnp.int32)
    img_index = jnp.arange(SEQ - PATCH_TOK, dtype=jnp.int32)
    img_ids = jnp.stack([jnp.zeros_like(img_index) + frame_idx, row_off + img_index // GRID_W, col_off + img_index % GRID_W], axis=-1)
    txt_ids = jnp.zeros((PATCH_TOK, 3), jnp.int32)
    return jnp.concatenate([txt_ids, img_ids], axis=0).reshape(PATCHES, PATCH_TOK, 3)


def setup_inputs(seed: int = 0, part: int = 0) -> dict:
    shared = jax.random.split(jax.random.key(seed), 8)
    own_keys = jax.random.split(jax.random.fold_in(jax.random.key(seed + 1), part), 4)
    proj_dim = 3 * WIDTH + MLP_DIM
    act_shape = (BATCH, PATCHES, PATCH_TOK, WIDTH)
    buf_shape = (LAYERS, BATCH, PATCHES, PATCH_TOK, WIDTH)
    row_gain = jnp.where(jnp.arange(WIDTH + MLP_DIM) < WIDTH, 2.0, 1.0)[None, :, None]
    return {
        'x_in': jax.random.normal(own_keys[0], act_shape, jnp.float32).astype(jnp.bfloat16),
        'cond_vec': jax.random.normal(own_keys[1], (BATCH, WIDTH), jnp.float32).astype(jnp.bfloat16),
        'pos_ids': make_ids(shared[0]),
        'w_mod': (jax.random.normal(shared[1], (LAYERS, WIDTH, 3 * WIDTH), jnp.float32) * WIDTH ** -0.5).astype(jnp.bfloat16),
        'b_mod': (0.5 * jax.random.normal(shared[2], (LAYERS, 3 * WIDTH), jnp.float32)).astype(jnp.bfloat16),
        'w_one': (jax.random.normal(shared[3], (LAYERS, WIDTH, proj_dim), jnp.float32) * WIDTH ** -0.5).astype(jnp.bfloat16),
        'b_one': (0.5 * jax.random.normal(shared[4], (LAYERS, proj_dim), jnp.float32)).astype(jnp.bfloat16),
        'qk_scale': (QK_GAIN * (1.0 + 0.3 * jax.random.normal(shared[5], (LAYERS, 2, HEAD_DIM), jnp.float32))).astype(jnp.bfloat16),
        'w_two': (jax.random.normal(shared[6], (LAYERS, WIDTH + MLP_DIM, WIDTH), jnp.float32) * (WIDTH + MLP_DIM) ** -0.5 * row_gain).astype(jnp.bfloat16),
        'b_two': (0.5 * jax.random.normal(shared[7], (LAYERS, WIDTH), jnp.float32)).astype(jnp.bfloat16),
        'k_prev': (QK_GAIN * jax.random.normal(own_keys[2], buf_shape, jnp.float32)).astype(jnp.bfloat16),
        'v_prev': jax.random.normal(own_keys[3], buf_shape, jnp.float32).astype(jnp.bfloat16),
    }


def layer_norm(hidden):
    act32 = hidden.astype(jnp.float32)
    centered = act32 - jnp.mean(act32, axis=-1, keepdims=True)
    return centered * lax.rsqrt(jnp.mean(centered * centered, axis=-1, keepdims=True) + 1e-6)


def rope_tables(pos_ids, head_dim):
    axis_zero = head_dim // 8
    axis_rest = (head_dim - axis_zero) // 2
    pieces = []
    for axis_idx, axis_dim in enumerate((axis_zero, axis_rest, head_dim - axis_zero - axis_rest)):
        axis_freqs = 1.0 / (10000.0 ** (jnp.arange(0, axis_dim, 2, dtype=jnp.float32) / axis_dim))
        pieces.append(pos_ids[..., axis_idx:axis_idx + 1].astype(jnp.float32) * axis_freqs)
    angles = jnp.concatenate(pieces, axis=-1)[..., None, :]
    return jnp.cos(angles), jnp.sin(angles)


def rms_rope(raw_heads, norm_gain, cos_tab, sin_tab):
    raw32 = raw_heads.astype(jnp.float32)
    normed = raw32 * lax.rsqrt(jnp.mean(raw32 * raw32, axis=-1, keepdims=True) + 1e-6) * norm_gain.astype(jnp.float32)
    pair_view = normed.reshape(normed.shape[:-1] + (normed.shape[-1] // 2, 2))
    even_part = pair_view[..., 0]
    odd_part = pair_view[..., 1]
    rotated = jnp.stack([cos_tab * even_part - sin_tab * odd_part, sin_tab * even_part + cos_tab * odd_part], axis=-1)
    return rotated.reshape(raw_heads.shape).astype(jnp.bfloat16)


def reference(x_in, cond_vec, pos_ids, w_mod, b_mod, w_one, b_one, qk_scale, w_two, b_two, k_prev, v_prev):
    batch_size, patches, patch_tok, width = x_in.shape
    head_dim = qk_scale.shape[-1]
    head_count = width // head_dim
    seq_len = patches * patch_tok
    score_scale = 1.0 / math.sqrt(head_dim)
    head_shape = (batch_size, patches, patch_tok, head_count, head_dim)
    cos_tab, sin_tab = rope_tables(pos_ids, head_dim)
    cond_act = jax.nn.silu(cond_vec.astype(jnp.float32)).astype(jnp.bfloat16)
    patch_rank = jnp.arange(patches)

    def layer_step(hidden, layer_in):
        mod_w, mod_b, one_w, one_b, norm_gain, two_w, two_b, k_old, v_old = layer_in
        mod_vals = (jnp.dot(cond_act, mod_w, preferred_element_type=jnp.float32) + mod_b.astype(jnp.float32))[:, None, None, :]
        shift_mod = mod_vals[..., :width]
        scale_mod = mod_vals[..., width:2 * width]
        gate_mod = mod_vals[..., 2 * width:]
        h_mod = (layer_norm(hidden) * (1.0 + scale_mod) + shift_mod).astype(jnp.bfloat16)
        proj_out = (jnp.dot(h_mod.reshape(-1, width), one_w, preferred_element_type=jnp.float32) + one_b.astype(jnp.float32)).astype(jnp.bfloat16)
        proj_out = proj_out.reshape(batch_size, patches, patch_tok, -1)
        q_rot = rms_rope(proj_out[..., :width].reshape(head_shape), norm_gain[0], cos_tab, sin_tab)
        k_rot = rms_rope(proj_out[..., width:2 * width].reshape(head_shape), norm_gain[1], cos_tab, sin_tab)
        v_new = proj_out[..., 2 * width:3 * width].reshape(head_shape)
        k_prior = k_old.reshape(head_shape)
        v_prior = v_old.reshape(head_shape)

        def attend(patch_idx):
            is_fresh = (patch_rank <= patch_idx)[None, :, None, None, None]
            key_all = jnp.where(is_fresh, k_rot, k_prior).reshape(batch_size, seq_len, head_count, head_dim).astype(jnp.float32)
            val_all = jnp.where(is_fresh, v_new, v_prior).reshape(batch_size, seq_len, head_count, head_dim).astype(jnp.float32)
            q_patch = lax.dynamic_index_in_dim(q_rot, patch_idx, axis=1, keepdims=False).astype(jnp.float32)
            scores = jnp.einsum('bqhd,bkhd->bhqk', q_patch, key_all) * score_scale
            prob_bf = jax.nn.softmax(scores, axis=-1).astype(jnp.bfloat16)
            return jnp.einsum('bhqk,bkhd->bqhd', prob_bf.astype(jnp.float32), val_all).astype(jnp.bfloat16)

        attn_out = jnp.moveaxis(lax.map(attend, patch_rank), 0, 1).reshape(x_in.shape)
        mlp_act = jax.nn.gelu(proj_out[..., 3 * width:].astype(jnp.float32), approximate=True).astype(jnp.bfloat16)
        joined = jnp.concatenate([attn_out, mlp_act], axis=-1).reshape(-1, two_w.shape[0])
        block_out = jnp.dot(joined, two_w, preferred_element_type=jnp.float32).reshape(x_in.shape) + two_b.astype(jnp.float32)
        hidden_new = (hidden.astype(jnp.float32) + gate_mod * block_out).astype(jnp.bfloat16)
        return hidden_new, (k_rot.reshape(x_in.shape), v_new.reshape(x_in.shape))

    x_out, (k_new, v_new) = lax.scan(layer_step, x_in, (w_mod, b_mod, w_one, b_one, qk_scale, w_two, b_two, k_prev, v_prev))
    return x_out, k_new, v_new
```

```python
import functools
import math

import jax
import jax.numpy as jnp
from jax import lax
from jax.experimental import pallas as pl
from jax.experimental.pallas import tpu as pltpu
from jax.sharding import PartitionSpec as P

MESH = pl.DeviceIdType.MESH
F32 = jnp.float32
BF16 = jnp.bfloat16
LOG2E = 1.4426950408889634


def mm(a, b):
    return jnp.dot(a, b, preferred_element_type=F32)


def gelu(u):
    inner = u * (0.7978845608028654 + 0.035677408136300125 * (u * u))
    half = 0.5 * u
    return half + half * jnp.tanh(inner)


def block_kernel(dims, x_hbm, w1_hbm, w2_hbm, kp_hbm, vp_hbm, cos_hbm, sin_hbm, modp, b1, gains, ones,
                 xo_hbm, kn_hbm, vn_hbm,
                 w1, w2a, w2s, kbuf, vt, sbuf, qrhs, h, xs, snd, acc, attn, vst, tab,
                 w1_sem, wm_sem, w2a_sem, w2s_sem, kp_sem, vp_sem, x_sem, snd_sem, xo_sem, kn_sem, vn_sem, tab_sem, credit):
    stages, patches, tok, width, mlp, hd = dims
    seq = patches * tok
    pair = 2 * hd
    pairs = width // pair
    qkv = 3 * width
    mcol = mlp // pairs
    slots = w2s.shape[0]
    per = patches // stages
    expc = LOG2E / math.sqrt(hd)
    stage = lax.axis_index('pp') if stages > 1 else jnp.int32(0)
    last = stages - 1

    def w1_copy(j):
        cols = pl.ds(j * (qkv // 3), qkv // 3)
        return pltpu.make_async_copy(w1_hbm.at[:, cols], w1.at[:, cols], w1_sem.at[j])

    def wm_copy(i):
        cols = pl.ds(pl.multiple_of(qkv + i * mcol, mcol), mcol)
        return pltpu.make_async_copy(w1_hbm.at[:, cols], w1.at[:, cols], wm_sem.at[i])

    def w2s_copy(i, slot):
        return pltpu.make_async_copy(w2_hbm.at[pl.ds(pl.multiple_of(width + i * mcol, mcol), mcol), :], w2s.at[slot], w2s_sem.at[slot])

    w2a_copy = pltpu.make_async_copy(w2_hbm.at[pl.ds(0, width), :], w2a, w2a_sem)
    kp_copy = pltpu.make_async_copy(kp_hbm.at[pl.ds(tok, seq - tok), :], kbuf.at[pl.ds(tok, seq - tok), :], kp_sem)

    vrows = mcol
    vparts = seq // vrows

    def vp_copy(p):
        return pltpu.make_async_copy(vp_hbm.at[pl.ds(p * vrows, vrows), :], w2s.at[p % slots], vp_sem.at[p % slots])

    def x_copy(m, slot):
        return pltpu.make_async_copy(x_hbm.at[m], xs.at[slot], x_sem.at[slot])

    def tab_copies(m, slot):
        return (pltpu.make_async_copy(cos_hbm.at[m], tab.at[slot, 0], tab_sem.at[slot, 0]),
                pltpu.make_async_copy(sin_hbm.at[m], tab.at[slot, 1], tab_sem.at[slot, 1]))

    def kn_copy(m, slot):
        rows = pl.ds(pl.multiple_of(m * tok, tok), tok)
        return pltpu.make_async_copy(kbuf.at[rows, :], kn_hbm.at[rows, :], kn_sem.at[slot])

    def vn_copy(m, slot):
        rows = pl.ds(pl.multiple_of(m * tok, tok), tok)
        return pltpu.make_async_copy(vst.at[slot], vn_hbm.at[rows, :], vn_sem.at[slot])

    def send_copy(slot):
        return pltpu.make_async_remote_copy(
            src_ref=snd.at[slot], dst_ref=xs.at[slot], send_sem=snd_sem.at[slot], recv_sem=x_sem.at[slot],
            device_id={'pp': jnp.minimum(stage + 1, last)}, device_id_type=MESH)

    def give_copy(slot, owner, place):
        return pltpu.make_async_remote_copy(
            src_ref=snd.at[slot], dst_ref=xo_hbm.at[place], send_sem=snd_sem.at[slot], recv_sem=xo_sem.at[place],
            device_id={'pp': owner}, device_id_type=MESH)

    def keep_copy(slot, place):
        return pltpu.make_async_copy(snd.at[slot], xo_hbm.at[place], snd_sem.at[slot])

    if stages > 1:
        barrier = pltpu.get_barrier_semaphore()

        def greet(d, c):
            pl.semaphore_signal(barrier, inc=1, device_id={'pp': lax.rem(stage + d, stages)}, device_id_type=MESH)
            return c
        lax.fori_loop(1, stages, greet, 0)

    @pl.when(stage == 0)
    def _():
        x_copy(0, 0).start()
        x_copy(1, 1).start()
    for c in tab_copies(0, 0):
        c.start()
    for j in range(3):
        w1_copy(j).start()
    for p in range(slots):
        vp_copy(p).start()
    kp_copy.start()
    for i in range(pairs):
        wm_copy(i).start()
    w2a_copy.start()

    qrhs[...] = jnp.zeros_like(qrhs)
    if stages > 1:
        pl.semaphore_wait(barrier, stages - 1)

    def patch_step(m, carry):
        slot = lax.rem(m, 2)
        rows = pl.ds(pl.multiple_of(m * tok, tok), tok)
        x_copy(0, slot).wait()
        for c in tab_copies(0, slot):
            c.wait()

        @pl.when(m + 1 < patches)
        def _():
            for c in tab_copies(m + 1, 1 - slot):
                c.start()

        xv = xs[slot].astype(F32)
        cen = xv - jnp.mean(xv, axis=1, keepdims=True)
        nrm = cen * lax.rsqrt(jnp.mean(cen * cen, axis=1, keepdims=True) + 1e-6)
        h[...] = (nrm * modp[1:2, :] + modp[0:1, :]).astype(BF16)
        acc[...] = jnp.zeros_like(acc)

        @pl.when(m == 0)
        def _():
            for j in range(3):
                w1_copy(j).wait()

        @pl.when(m >= 2)
        def _():
            vn_copy(0, slot).wait()
            kn_copy(0, slot).wait()

        lane = lax.broadcasted_iota(jnp.int32, (tok, pair), 1)
        even = (lane % 2) == 0
        cos_t = tab[slot, 0]
        sin_t = tab[slot, 1]

        def head_norm(raw, ga, gb):
            r32 = raw.astype(F32)
            sq = r32 * r32
            hi = sq.astype(BF16)
            lo = (sq - hi.astype(F32)).astype(BF16)
            ssq = mm(hi, ones[...]) + mm(lo, ones[...])
            inv = lax.rsqrt(ssq * (1.0 / hd) + 1e-6)
            outs = []
            for t in range(2):
                part = r32[:, t * pair:(t + 1) * pair]
                other = jnp.where(even, pltpu.roll(part, pair - 1, 1), pltpu.roll(part, 1, 1))
                outs.append(((part * ga + other * gb) * inv[:, t * pair:(t + 1) * pair]).astype(BF16))
            return outs

        gq = cos_t * gains[0:1, :]
        gqs = sin_t * gains[1:2, :]
        gk = cos_t * gains[2:3, :]
        gks = sin_t * gains[3:4, :]
        blk = 2 * pair

        def qkv_step(j, c):
            def proj(base):
                cols = pl.ds(pl.multiple_of(base + j * blk, blk), blk)
                return (mm(h[...], w1[:, cols]) + b1[:, cols]).astype(BF16)
            raw_q = proj(0)
            raw_k = proj(width)
            raw_v = proj(2 * width)
            vst[slot, :, pl.ds(pl.multiple_of(j * blk, blk), blk)] = raw_v
            vt[pl.ds(pl.multiple_of(j * blk, blk), blk), rows] = raw_v.T
            q2 = head_norm(raw_q, gq, gqs)
            k2 = head_norm(raw_k, gk, gks)
            for t in range(2):
                qt = q2[t].T
                qrhs[2 * j + t, 0:hd, 0:tok] = qt[0:hd, :]
                qrhs[2 * j + t, hd:pair, tok:2 * tok] = qt[hd:pair, :]
                kbuf[rows, pl.ds(pl.multiple_of(j * blk + t * pair, pair), pair)] = k2[t]
            return c
        lax.fori_loop(0, width // blk, qkv_step, 0)

        kn_copy(m, slot).start()
        vn_copy(m, slot).start()

        @pl.when(m == 0)
        def _():
            for p in range(vparts):
                vp_copy(p).wait()

                def turn(d, c, p=p):
                    ds = pl.ds(pl.multiple_of(d * pair, pair), pair)
                    for t in range(vrows // tok):
                        if p * vrows + t * tok >= tok:
                            vt[ds, pl.ds(p * vrows + t * tok, tok)] = w2s[p % slots, pl.ds(t * tok, tok), ds].T
                    return c
                lax.fori_loop(0, pairs, turn, 0)
                if p + slots < vparts:
                    vp_copy(p + slots).start()
            for i in range(slots - 1):
                w2s_copy(i, i).start()
            kp_copy.wait()

        def pair_step(i, c):
            ws = lax.rem(i, slots)
            w2s_copy(0, ws).wait()

            @pl.when(m == 0)
            def _():
                wm_copy(i).wait()
            nxt = i + slots - 1

            @pl.when(jnp.logical_or(m + 1 < patches, nxt < pairs))
            def _():
                w2s_copy(lax.rem(nxt, pairs), lax.rem(nxt, slots)).start()
            lanes = pl.ds(pl.multiple_of(i * pair, pair), pair)
            rhs = qrhs[i]
            ck = 2 * tok
            top = None
            for b in range(seq // ck):
                s = mm(kbuf[b * ck:(b + 1) * ck, lanes], rhs)
                sbuf[b * ck:(b + 1) * ck, :] = s
                t8 = jnp.max(s.reshape(ck // 8, 8, 2 * tok), axis=0)
                top = t8 if top is None else jnp.maximum(top, t8)
            top = jnp.max(top, axis=0, keepdims=True)
            mcols = pl.ds(pl.multiple_of(qkv + i * mcol, mcol), mcol)
            up = (mm(h[...], w1[:, mcols]) + b1[:, mcols]).astype(BF16)
            act = gelu(up.astype(F32)).astype(BF16)
            acc[...] += mm(act, w2s[ws])
            tot = None
            out = None
            for b in range(seq // ck):
                e = jnp.exp2((sbuf[b * ck:(b + 1) * ck, :] - top) * expc)
                l8 = jnp.sum(e.reshape(ck // 8, 8, 2 * tok), axis=0)
                tot = l8 if tot is None else tot + l8
                o = mm(vt[lanes, b * ck:(b + 1) * ck], e.astype(BF16))
                out = o if out is None else out + o
            inv = 1.0 / jnp.sum(tot, axis=0, keepdims=True)
            both = jnp.concatenate([out[0:hd, 0:tok] * inv[:, 0:tok], out[hd:pair, tok:2 * tok] * inv[:, tok:2 * tok]], axis=0)
            attn[:, lanes] = both.astype(BF16).T
            return c
        lax.fori_loop(0, pairs, pair_step, 0)

        @pl.when(m == 0)
        def _():
            w2a_copy.wait()

        @pl.when(m >= 2)
        def _():
            if stages > 1:
                @pl.when(stage < last)
                def _():
                    send_copy(slot).wait_send()
                    pl.semaphore_wait(credit, 1)

                @pl.when(stage == last)
                def _():
                    keep_copy(slot, 0).wait()
            else:
                keep_copy(slot, 0).wait()

        for n in range(width // blk):
            cols = slice(n * blk, (n + 1) * blk)
            o = mm(attn[...], w2a[:, cols]) + acc[:, cols] + modp[3:4, cols]
            snd[slot, :, cols] = (xs[slot, :, cols].astype(F32) + modp[2:3, cols] * o).astype(BF16)

        if stages > 1:
            @pl.when(stage < last)
            def _():
                send_copy(slot).start()

            @pl.when(stage == last)
            def _():
                owner = m // per

                @pl.when(owner < last)
                def _():
                    give_copy(slot, jnp.minimum(owner, last - 1), lax.rem(m, per)).start()

                @pl.when(owner == last)
                def _():
                    keep_copy(slot, lax.rem(m, per)).start()

            @pl.when(jnp.logical_and(stage > 0, m + 2 < patches))
            def _():
                pl.semaphore_signal(credit, inc=1, device_id={'pp': jnp.maximum(stage - 1, 0)}, device_id_type=MESH)
        else:
            keep_copy(slot, m).start()

        @pl.when(jnp.logical_and(stage == 0, m + 2 < patches))
        def _():
            x_copy(m + 2, slot).start()
        return carry

    lax.fori_loop(0, patches, patch_step, 0)

    for slot in range(2):
        kn_copy(0, slot).wait()
        vn_copy(0, slot).wait()
        if stages > 1:
            @pl.when(stage < last)
            def _():
                send_copy(slot).wait_send()

            @pl.when(stage == last)
            def _():
                keep_copy(slot, 0).wait()
        else:
            keep_copy(slot, 0).wait()
    if stages > 1:
        @pl.when(stage < last)
        def _():
            for place in range(per):
                give_copy(0, 0, place).wait_recv()


def rope_rows(pos_ids, head_dim):
    axis_zero = head_dim // 8
    axis_rest = (head_dim - axis_zero) // 2
    pieces = []
    for axis_idx, axis_dim in enumerate((axis_zero, axis_rest, head_dim - axis_zero - axis_rest)):
        axis_freqs = 1.0 / (10000.0 ** (jnp.arange(0, axis_dim, 2, dtype=F32) / axis_dim))
        pieces.append(pos_ids[..., axis_idx:axis_idx + 1].astype(F32) * axis_freqs)
    angles = jnp.concatenate(pieces, axis=-1)
    cos = jnp.repeat(jnp.cos(angles), 2, axis=-1)
    sin = jnp.sin(angles)
    sin = jnp.stack([-sin, sin], axis=-1).reshape(cos.shape)
    return jnp.concatenate([cos, cos], axis=-1), jnp.concatenate([sin, sin], axis=-1)


def make_stage(stages):
    def stage_program(x_in, cond_vec, pos_ids, w_mod, b_mod, w_one, b_one, qk_scale, w_two, b_two, k_prev, v_prev):
        batch, patches, tok, width = x_in.shape
        hd = qk_scale.shape[-1]
        mlp = w_two.shape[1] - width
        seq = patches * tok
        pair = 2 * hd
        pairs = width // pair
        mcol = mlp // pairs
        per = patches // stages
        cond_act = jax.nn.silu(cond_vec.astype(F32)).astype(BF16)
        mod = jnp.dot(cond_act, w_mod[0], preferred_element_type=F32)[0] + b_mod[0].astype(F32)
        modp = jnp.stack([mod[:width], 1.0 + mod[width:2 * width], mod[2 * width:], b_two[0].astype(F32)])
        cos_t, sin_t = rope_rows(pos_ids, hd)
        g = qk_scale[0].astype(F32)
        gsw = g.reshape(2, hd // 2, 2)[:, :, ::-1].reshape(2, hd)
        gains = jnp.stack([g[0], gsw[0], g[1], gsw[1]])
        gains = jnp.concatenate([gains, gains], axis=1)
        head_id = jnp.arange(2 * pair) // hd
        ones = (head_id[:, None] == head_id[None, :]).astype(BF16)
        hbm = functools.partial(pltpu.with_memory_space_constraint, memory_space=pltpu.HBM)
        dims = (stages, patches, tok, width, mlp, hd)
        out_patches = per
        x_out, k_new, v_new = pl.pallas_call(
            functools.partial(block_kernel, dims),
            out_shape=(jax.ShapeDtypeStruct((out_patches, tok, width), BF16),
                       jax.ShapeDtypeStruct((seq, width), BF16), jax.ShapeDtypeStruct((seq, width), BF16)),
            in_specs=[pl.BlockSpec(memory_space=pltpu.HBM)] * 7 + [pl.BlockSpec(memory_space=pltpu.VMEM)] * 4,
            out_specs=(pl.BlockSpec(memory_space=pltpu.HBM),) * 3,
            scratch_shapes=[
                pltpu.VMEM((width, 3 * width + mlp), BF16),
                pltpu.VMEM((width, width), BF16),
                pltpu.VMEM((3, mcol, width), BF16),
                pltpu.VMEM((seq, width), BF16),
                pltpu.VMEM((width, seq), BF16),
                pltpu.VMEM((seq, 2 * tok), F32),
                pltpu.VMEM((pairs, pair, 2 * tok), BF16),
                pltpu.VMEM((tok, width), BF16),
                pltpu.VMEM((2, tok, width), BF16),
                pltpu.VMEM((2, tok, width), BF16),
                pltpu.VMEM((tok, width), F32),
                pltpu.VMEM((tok, width), BF16),
                pltpu.VMEM((2, tok, width), BF16),
                pltpu.VMEM((2, 2, tok, pair), F32),
                pltpu.SemaphoreType.DMA((3,)),
                pltpu.SemaphoreType.DMA((pairs,)),
                pltpu.SemaphoreType.DMA,
                pltpu.SemaphoreType.DMA((3,)),
                pltpu.SemaphoreType.DMA,
                pltpu.SemaphoreType.DMA((3,)),
                pltpu.SemaphoreType.DMA((2,)),
                pltpu.SemaphoreType.DMA((2,)),
                pltpu.SemaphoreType.DMA((per,)),
                pltpu.SemaphoreType.DMA((2,)),
                pltpu.SemaphoreType.DMA((2,)),
                pltpu.SemaphoreType.DMA((2, 2)),
                pltpu.SemaphoreType.REGULAR,
            ],
            compiler_params=pltpu.CompilerParams(
                vmem_limit_bytes=67043328, **(dict(collective_id=0, has_side_effects=True) if stages > 1 else {})),
            name='blocks',
        )(hbm(x_in[0]), hbm(w_one[0]), hbm(w_two[0]), hbm(k_prev.reshape(seq, width)), hbm(v_prev.reshape(seq, width)),
          hbm(cos_t), hbm(sin_t), modp, b_one.astype(F32), gains, ones)
        return x_out[None], k_new.reshape(k_prev.shape), v_new.reshape(v_prev.shape)
    return stage_program


def solution(mesh):
    stages = mesh.shape['pp']
    return jax.shard_map(
        make_stage(stages), mesh=mesh,
        in_specs=(P('dp'), P('dp'), P(), P('pp'), P('pp'), P('pp'), P('pp'), P('pp'), P('pp'), P('pp'), P('pp', 'dp'), P('pp', 'dp')),
        out_specs=(P('dp', 'pp'), P('pp', 'dp'), P('pp', 'dp')),
        check_vma=False)
```

```python
import functools
import math

import jax
import jax.numpy as jnp
from jax import lax
from jax.experimental import pallas as pl
from jax.experimental.pallas import tpu as pltpu
from jax.sharding import PartitionSpec as P

MESH = pl.DeviceIdType.MESH
F32 = jnp.float32
BF16 = jnp.bfloat16
LOG2E = 1.4426950408889634


DOWNS = (0, 1, 4, 8, 9, 12, 16, 17, 20)
LASTS = (2, 4, 6, 16, 17, 18, 20, 21, 22)
UPS = (2, 3, 4, 5, 6, 7)


def mm(a, b):
    return jnp.dot(a, b, preferred_element_type=F32)


def gelu(u):
    inner = u * (0.7978845608028654 + 0.035677408136300125 * (u * u))
    half = 0.5 * u
    return half + half * jnp.tanh(inner)


def block_kernel(dims, x_hbm, w1_hbm, w2_hbm, kp_hbm, vp_hbm, cos_hbm, sin_hbm, modp, b1, gains, ones,
                 xo_hbm, kn_hbm, vn_hbm,
                 w1, w2s, kbuf, vt, sbufs, tops, parts, acts, qrhs, h, xs, snd, acc, attn, vst, tab,
                 w1_sem, wm_sem, w2s_sem, kp_sem, vp_sem, x_sem, snd_sem, xo_sem, kn_sem, vn_sem, tab_sem, credit):
    stages, patches, tok, width, mlp, hd = dims
    seq = patches * tok
    pair = 2 * hd
    pairs = width // pair
    qkv = 3 * width
    mcol = mlp // pairs
    group = 3
    bodies = pairs // group
    span = group * mcol
    per = patches // stages
    expc = LOG2E / math.sqrt(hd)
    stage = lax.axis_index('pp') if stages > 1 else jnp.int32(0)
    last = stages - 1

    def w1_copy(j):
        cols = pl.ds(j * (qkv // 3), qkv // 3)
        return pltpu.make_async_copy(w1_hbm.at[:, cols], w1.at[:, cols], w1_sem.at[j])

    def wm_copy(j):
        if isinstance(j, int):
            lo = 0 if j == 0 else j * span + mcol
            cols = pl.ds(qkv + lo, min((j + 1) * span + mcol, mlp) - lo)
        else:
            cols = pl.ds(pl.multiple_of(qkv + j * span + mcol, mcol), span)
        return pltpu.make_async_copy(w1_hbm.at[:, cols], w1.at[:, cols], wm_sem.at[j])

    def w2_copy(par, j):
        row = j * span + width if j < bodies else 0
        return pltpu.make_async_copy(w2_hbm.at[pl.ds(row, span), :], w2s.at[par], w2s_sem.at[par])

    def w2_next(par, j):
        row = pl.multiple_of(j * span + width, mcol)
        return pltpu.make_async_copy(w2_hbm.at[pl.ds(row, span), :], w2s.at[par], w2s_sem.at[par])

    kp_copy = pltpu.make_async_copy(kp_hbm.at[pl.ds(tok, seq - tok), :], kbuf.at[pl.ds(tok, seq - tok), :], kp_sem)

    vrows = mcol
    vparts = seq // vrows

    def vp_part(p):
        return divmod(p * vrows, span)

    def vp_copy(p):
        par, row = vp_part(p)
        return pltpu.make_async_copy(vp_hbm.at[pl.ds(p * vrows, vrows), :], w2s.at[par, pl.ds(row, vrows), :], vp_sem.at[p])

    def x_copy(m, slot):
        return pltpu.make_async_copy(x_hbm.at[m], xs.at[slot], x_sem.at[slot])

    def tab_copies(m, slot):
        return (pltpu.make_async_copy(cos_hbm.at[m], tab.at[slot, 0], tab_sem.at[slot, 0]),
                pltpu.make_async_copy(sin_hbm.at[m], tab.at[slot, 1], tab_sem.at[slot, 1]))

    def kn_copy(m):
        rows = pl.ds(pl.multiple_of(m * tok, tok), tok)
        return pltpu.make_async_copy(kbuf.at[rows, :], kn_hbm.at[rows, :], kn_sem)

    def vn_copy(m):
        rows = pl.ds(pl.multiple_of(m * tok, tok), tok)
        return pltpu.make_async_copy(vst, vn_hbm.at[rows, :], vn_sem)

    def send_copy(slot):
        return pltpu.make_async_remote_copy(
            src_ref=snd, dst_ref=xs.at[slot], send_sem=snd_sem, recv_sem=x_sem.at[slot],
            device_id={'pp': jnp.minimum(stage + 1, last)}, device_id_type=MESH)

    def give_copy(owner, place):
        return pltpu.make_async_remote_copy(
            src_ref=snd, dst_ref=xo_hbm.at[place], send_sem=snd_sem, recv_sem=xo_sem.at[place],
            device_id={'pp': owner}, device_id_type=MESH)

    def keep_copy(place):
        return pltpu.make_async_copy(snd, xo_hbm.at[place], snd_sem)

    if stages > 1:
        barrier = pltpu.get_barrier_semaphore()

        def greet(d, c):
            pl.semaphore_signal(barrier, inc=1, device_id={'pp': lax.rem(stage + d, stages)}, device_id_type=MESH)
            return c
        lax.fori_loop(1, stages, greet, 0)

    @pl.when(stage == 0)
    def _():
        x_copy(0, 0).start()
        x_copy(1, 1).start()
    for c in tab_copies(0, 0):
        c.start()
    for j in range(3):
        w1_copy(j).start()
    for p in range(vparts):
        vp_copy(p).start()
    kp_copy.start()
    wm_copy(0).start()

    qrhs[...] = jnp.zeros_like(qrhs)
    for p in range(vparts):
        vp_copy(p).wait()
        par, row = vp_part(p)

        def turn(d, c, p=p, par=par, row=row):
            ds = pl.ds(pl.multiple_of(d * pair, pair), pair)
            for t in range(vrows // tok):
                if p * vrows + t * tok >= tok:
                    vt[ds, pl.ds(p * vrows + t * tok, tok)] = w2s[par, pl.ds(row + t * tok, tok), ds].T
            return c
        lax.fori_loop(0, pairs, turn, 0)
    w2_copy(0, 0).start()
    for j in range(1, bodies):
        wm_copy(j).start()
    kp_copy.wait()
    for j in range(3):
        w1_copy(j).wait()
    wm_copy(0).wait()

    if stages > 1:
        pl.semaphore_wait(barrier, stages - 1)

    def patch_step(m, carry):
        slot = lax.rem(m, 2)
        rows = pl.ds(pl.multiple_of(m * tok, tok), tok)
        x_copy(0, slot).wait()
        for c in tab_copies(0, slot):
            c.wait()

        @pl.when(m + 1 < patches)
        def _():
            for c in tab_copies(m + 1, 1 - slot):
                c.start()

        @pl.when(m >= 1)
        def _():
            vn_copy(0).wait()
            kn_copy(0).wait()

        w2_copy(lax.rem(m, 2), 0).wait()
        w2_copy(lax.rem(m + 1, 2), 1).start()

        xv = xs[slot].astype(F32)
        cen = xv - jnp.mean(xv, axis=1, keepdims=True)
        nrm = cen * lax.rsqrt(jnp.mean(cen * cen, axis=1, keepdims=True) + 1e-6)
        h[...] = (nrm * modp[1:2, :] + modp[0:1, :]).astype(BF16)
        acc[...] = jnp.zeros_like(acc)

        lane = lax.broadcasted_iota(jnp.int32, (tok, pair), 1)
        even = (lane % 2) == 0
        cos_t = tab[slot, 0]
        sin_t = tab[slot, 1]

        def head_norm(raw, ga, gb):
            r32 = raw.astype(F32)
            sq = r32 * r32
            hi = sq.astype(BF16)
            lo = (sq - hi.astype(F32)).astype(BF16)
            ssq = mm(hi, ones[...]) + mm(lo, ones[...])
            inv = lax.rsqrt(ssq * (1.0 / hd) + 1e-6)
            outs = []
            for t in range(2):
                part = r32[:, t * pair:(t + 1) * pair]
                other = jnp.where(even, pltpu.roll(part, pair - 1, 1), pltpu.roll(part, 1, 1))
                outs.append(((part * ga + other * gb) * inv[:, t * pair:(t + 1) * pair]).astype(BF16))
            return outs

        gq = cos_t * gains[0:1, :]
        gqs = sin_t * gains[1:2, :]
        gk = cos_t * gains[2:3, :]
        gks = sin_t * gains[3:4, :]
        blk = 2 * pair

        wide = 2 * blk

        def proj(base, j):
            cols = slice(base + j * wide, base + (j + 1) * wide)
            return (mm(h[...], w1[:, cols]) + b1[:, cols]).astype(BF16)

        def put_q(raw, j):
            for i in range(2):
                q2 = head_norm(raw[:, i * blk:(i + 1) * blk], gq, gqs)
                for t in range(2):
                    n = 4 * j + 2 * i + t
                    q32 = q2[t].astype(F32) * expc
                    hi = q32.astype(BF16)
                    lo = (q32 - hi.astype(F32)).astype(BF16)
                    for r, qt in ((0, hi.T), (pair, lo.T)):
                        qrhs[n, r:r + hd, 0:tok] = qt[0:hd, :]
                        qrhs[n, r + hd:r + pair, tok:2 * tok] = qt[hd:pair, :]

        def put_k(raw, j):
            for i in range(2):
                k2 = head_norm(raw[:, i * blk:(i + 1) * blk], gk, gks)
                for t in range(2):
                    n = 4 * j + 2 * i + t
                    kbuf[rows, n * pair:(n + 1) * pair] = k2[t]

        def put_v(raw, j):
            vst[:, j * wide:(j + 1) * wide] = raw
            vt[j * wide:(j + 1) * wide, rows] = raw.T

        ck = 2 * tok
        nck = seq // ck
        ring = 12
        lead = nck + 1

        def score(i, b, place):
            lanes = pl.ds(pl.multiple_of(i * pair, pair), pair)
            found = []
            for r in range(2):
                kc = kbuf[b * ck + r * tok:b * ck + (r + 1) * tok, lanes]
                v = mm(jnp.concatenate([kc, kc], axis=1), qrhs[i])
                sbufs[place, r * tok:(r + 1) * tok, :] = v
                found.append(jnp.max(v.reshape(tok // 8, 8, 2 * tok), axis=0))
            return jnp.maximum(found[0], found[1])

        def high(tops8):
            t8 = functools.reduce(jnp.maximum, tops8)
            return jnp.max(t8, axis=0, keepdims=True)

        work = []
        for j in range(width // wide):
            work += [(put_q, 0, j), (put_k, width, j)]
        work += [(put_v, 2 * width, j) for j in range(width // wide)]
        held = None
        for put, base, j in work:
            raw = proj(base, j)
            if held is not None:
                held[0](held[1], held[2])
            held = (put, raw, j)
            if put is put_v and j == 0:
                tops8 = [score(0, b, b) for b in range(nck)]
                tops8.append(score(1, 0, nck))
        steps = group * nck
        kp = width // ck

        def plan(final):
            places = {}
            for p in range(group):
                if not final or p < group - 1:
                    for k in range(kp):
                        places.setdefault(nck * p + UPS[k], []).append(('up', p, k))
                for k in range(kp // 2):
                    if final:
                        at = LASTS[p * 3 + k]
                    else:
                        at = DOWNS[p * 3 + k]
                    places.setdefault(at, []).append(('down', p, k))
            return places

        def up_piece(n, k):
            ks = slice(k * ck, (k + 1) * ck)
            return mm(h[:, ks], w1[ks, pl.ds(pl.multiple_of(qkv + n * mcol, mcol), mcol)])

        def activate(ups, n):
            up = (functools.reduce(jnp.add, ups) + b1[:, pl.ds(pl.multiple_of(qkv + n * mcol, mcol), mcol)]).astype(BF16)
            return gelu(up.astype(F32)).astype(BF16)

        def body(j, final, top, part, act0):
            par = lax.rem(m + j, 2)
            tops8 = [None] * nck + [part]
            places = plan(final)
            ups = []
            act = {0: act0}
            probs = None
            tots = []
            outs = []
            nexttop = None
            for t in range(steps + 1):
                u, b = divmod(t, nck)
                new = None
                if t < steps:
                    if b == 0 and u > 0:
                        top = nexttop
                    e = jnp.exp2(sbufs[t % ring] - top)
                    tots.append(jnp.sum(e.reshape(ck // 8, 8, 2 * tok), axis=0))
                    new = e.astype(BF16)
                    q = t + lead
                    if q < steps or not final:
                        tops8.append(score(group * j + q // nck, q % nck, q % ring))
                        if b == nck - 2:
                            nexttop = high(tops8[(u + 1) * nck:(u + 2) * nck])
                if t > 0:
                    pu, pb = divmod(t - 1, nck)
                    lanes = pl.ds(pl.multiple_of((group * j + pu) * pair, pair), pair)
                    outs.append(mm(vt[lanes, pb * ck:(pb + 1) * ck], probs))
                    if pb == nck - 1:
                        inv = 1.0 / jnp.sum(functools.reduce(jnp.add, tots[:nck]), axis=0, keepdims=True)
                        both = 0
                        for r in range(2):
                            out = functools.reduce(jnp.add, outs[r::2])
                            both = both + jnp.concatenate([out[0:hd, 0:tok] * inv[:, 0:tok], out[hd:pair, tok:2 * tok] * inv[:, tok:2 * tok]], axis=0)
                        attn[:, lanes] = both.astype(BF16).T
                        outs = []
                        tots = tots[nck:]
                probs = new
                for kind, p, k in places.get(t, ()):
                    if kind == 'up':
                        ups.append(up_piece(group * j + p + 1, k))
                        if k == kp - 1:
                            act[p + 1] = activate(ups, group * j + p + 1)
                            ups = []
                    else:
                        ks = slice(k * mcol, (k + 1) * mcol)
                        acc[:, ks] += mm(act[p], w2s[par, p * mcol:(p + 1) * mcol, ks])
            if not final:
                tops[...] = nexttop
                parts[...] = tops8[-1]
                acts[...] = act[group]

        act0 = activate([up_piece(0, k) for k in range(kp)], 0)
        held[0](held[1], held[2])
        body(0, False, high(tops8[:nck]), tops8[nck], act0)

        def start(j):
            @pl.when(m == 0)
            def _():
                wm_copy(j).wait()
            w2_copy(lax.rem(m + j, 2), 0).wait()

        def body_step(j, c):
            start(j)
            w2_next(lax.rem(m + j + 1, 2), j + 1).start()
            body(j, False, tops[...], parts[...], acts[...])
            return c
        lax.fori_loop(1, bodies - 1, body_step, 0)
        @pl.when(m >= 1)
        def _():
            if stages > 1:
                @pl.when(stage < last)
                def _():
                    send_copy(slot).wait_send()

                @pl.when(stage == last)
                def _():
                    keep_copy(0).wait()
            else:
                keep_copy(0).wait()

        if stages > 1:
            @pl.when(jnp.logical_and(stage < last, m >= 2))
            def _():
                pl.semaphore_wait(credit, 1)

        start(bodies - 1)
        w2_copy(lax.rem(m + bodies, 2), bodies).start()
        kn_copy(m).start()
        vn_copy(m).start()
        body(bodies - 1, True, tops[...], parts[...], acts[...])

        w2par = lax.rem(m + bodies, 2)
        w2_copy(w2par, 0).wait()

        w2_copy(1 - w2par, 0).start()

        sums = []
        cut = (pairs - 2) * pair
        for n in range(width // wide):
            cols = slice(n * wide, (n + 1) * wide)
            sums.append(mm(attn[:, 0:cut], w2s[w2par, 0:cut, cols]))
        for n in range(width // wide):
            cols = slice(n * wide, (n + 1) * wide)
            o = sums[n] + mm(attn[:, cut:width], w2s[w2par, cut:width, cols]) + acc[:, cols] + modp[3:4, cols]
            snd[:, cols] = (xs[slot, :, cols].astype(F32) + modp[2:3, cols] * o).astype(BF16)

        if stages > 1:
            @pl.when(stage < last)
            def _():
                send_copy(slot).start()

            @pl.when(stage == last)
            def _():
                owner = m // per

                @pl.when(owner < last)
                def _():
                    give_copy(jnp.minimum(owner, last - 1), lax.rem(m, per)).start()

                @pl.when(owner == last)
                def _():
                    keep_copy(lax.rem(m, per)).start()

            @pl.when(jnp.logical_and(stage > 0, m + 2 < patches))
            def _():
                pl.semaphore_signal(credit, inc=1, device_id={'pp': jnp.maximum(stage - 1, 0)}, device_id_type=MESH)
        else:
            keep_copy(m).start()

        @pl.when(jnp.logical_and(stage == 0, m + 2 < patches))
        def _():
            x_copy(m + 2, slot).start()
        return carry

    lax.fori_loop(0, patches, patch_step, 0)

    kn_copy(0).wait()
    vn_copy(0).wait()
    w2_copy(patches % 2, 0).wait()
    if stages > 1:
        @pl.when(stage < last)
        def _():
            send_copy(0).wait_send()
            for place in range(per):
                give_copy(0, place).wait_recv()

        @pl.when(stage == last)
        def _():
            keep_copy(0).wait()
    else:
        keep_copy(0).wait()


def rope_rows(pos_ids, head_dim):
    axis_zero = head_dim // 8
    axis_rest = (head_dim - axis_zero) // 2
    pieces = []
    for axis_idx, axis_dim in enumerate((axis_zero, axis_rest, head_dim - axis_zero - axis_rest)):
        axis_freqs = 1.0 / (10000.0 ** (jnp.arange(0, axis_dim, 2, dtype=F32) / axis_dim))
        pieces.append(pos_ids[..., axis_idx:axis_idx + 1].astype(F32) * axis_freqs)
    angles = jnp.concatenate(pieces, axis=-1)
    cos = jnp.repeat(jnp.cos(angles), 2, axis=-1)
    sin = jnp.sin(angles)
    sin = jnp.stack([-sin, sin], axis=-1).reshape(cos.shape)
    return jnp.concatenate([cos, cos], axis=-1), jnp.concatenate([sin, sin], axis=-1)


def make_stage(stages):
    def stage_program(x_in, cond_vec, pos_ids, w_mod, b_mod, w_one, b_one, qk_scale, w_two, b_two, k_prev, v_prev):
        batch, patches, tok, width = x_in.shape
        hd = qk_scale.shape[-1]
        mlp = w_two.shape[1] - width
        seq = patches * tok
        pair = 2 * hd
        pairs = width // pair
        mcol = mlp // pairs
        per = patches // stages
        cond_act = jax.nn.silu(cond_vec.astype(F32)).astype(BF16)
        mod = jnp.dot(cond_act, w_mod[0], preferred_element_type=F32)[0] + b_mod[0].astype(F32)
        modp = jnp.stack([mod[:width], 1.0 + mod[width:2 * width], mod[2 * width:], b_two[0].astype(F32)])
        cos_t, sin_t = rope_rows(pos_ids, hd)
        g = qk_scale[0].astype(F32)
        gsw = g.reshape(2, hd // 2, 2)[:, :, ::-1].reshape(2, hd)
        gains = jnp.stack([g[0], gsw[0], g[1], gsw[1]])
        gains = jnp.concatenate([gains, gains], axis=1)
        head_id = jnp.arange(2 * pair) // hd
        ones = (head_id[:, None] == head_id[None, :]).astype(BF16)
        hbm = functools.partial(pltpu.with_memory_space_constraint, memory_space=pltpu.HBM)
        dims = (stages, patches, tok, width, mlp, hd)
        out_patches = per
        x_out, k_new, v_new = pl.pallas_call(
            functools.partial(block_kernel, dims),
            out_shape=(jax.ShapeDtypeStruct((out_patches, tok, width), BF16),
                       jax.ShapeDtypeStruct((seq, width), BF16), jax.ShapeDtypeStruct((seq, width), BF16)),
            in_specs=[pl.BlockSpec(memory_space=pltpu.HBM)] * 7 + [pl.BlockSpec(memory_space=pltpu.VMEM)] * 4,
            out_specs=(pl.BlockSpec(memory_space=pltpu.HBM),) * 3,
            scratch_shapes=[
                pltpu.VMEM((width, 3 * width + mlp), BF16),
                pltpu.VMEM((2, 3 * mcol, width), BF16),
                pltpu.VMEM((seq, width), BF16),
                pltpu.VMEM((width, seq), BF16),
                pltpu.VMEM((12, 2 * tok, 2 * tok), F32),
                pltpu.VMEM((1, 2 * tok), F32),
                pltpu.VMEM((8, 2 * tok), F32),
                pltpu.VMEM((tok, mcol), BF16),
                pltpu.VMEM((pairs, 2 * pair, 2 * tok), BF16),
                pltpu.VMEM((tok, width), BF16),
                pltpu.VMEM((2, tok, width), BF16),
                pltpu.VMEM((tok, width), BF16),
                pltpu.VMEM((tok, width), F32),
                pltpu.VMEM((tok, width), BF16),
                pltpu.VMEM((tok, width), BF16),
                pltpu.VMEM((2, 2, tok, pair), F32),
                pltpu.SemaphoreType.DMA((3,)),
                pltpu.SemaphoreType.DMA((pairs // 3,)),
                pltpu.SemaphoreType.DMA((2,)),
                pltpu.SemaphoreType.DMA,
                pltpu.SemaphoreType.DMA((4,)),
                pltpu.SemaphoreType.DMA((2,)),
                pltpu.SemaphoreType.DMA,
                pltpu.SemaphoreType.DMA((per,)),
                pltpu.SemaphoreType.DMA,
                pltpu.SemaphoreType.DMA,
                pltpu.SemaphoreType.DMA((2, 2)),
                pltpu.SemaphoreType.REGULAR,
            ],
            compiler_params=pltpu.CompilerParams(
                vmem_limit_bytes=67043328, **(dict(collective_id=0, has_side_effects=True) if stages > 1 else {})),
            name='blocks',
        )(hbm(x_in[0]), hbm(w_one[0]), hbm(w_two[0]), hbm(k_prev.reshape(seq, width)), hbm(v_prev.reshape(seq, width)),
          hbm(cos_t), hbm(sin_t), modp, b_one.astype(F32), gains, ones)
        return x_out[None], k_new.reshape(k_prev.shape), v_new.reshape(v_prev.shape)
    return stage_program


def solution(mesh):
    stages = mesh.shape['pp']
    return jax.shard_map(
        make_stage(stages), mesh=mesh,
        in_specs=(P('dp'), P('dp'), P(), P('pp'), P('pp'), P('pp'), P('pp'), P('pp'), P('pp'), P('pp'), P('pp', 'dp'), P('pp', 'dp')),
        out_specs=(P('dp', 'pp'), P('pp', 'dp'), P('pp', 'dp')),
        check_vma=False)
```

```python
import functools
import math

import jax
import jax.numpy as jnp
import numpy as np
from jax import lax
from jax.experimental import pallas as pl
from jax.experimental.pallas import tpu as pltpu
from jax.sharding import PartitionSpec as P

MESH = pl.DeviceIdType.MESH
F32 = jnp.float32
BF16 = jnp.bfloat16
LOG2E = 1.4426950408889634


DOWNS = (0, 1, 4, 8, 9, 12, 16, 17, 20)
LASTS = (2, 4, 6, 16, 17, 18, 20, 21, 22)
UPS = (2, 3, 4, 5, 6, 7)


def mm(a, b):
    return jnp.dot(a, b, preferred_element_type=F32)


def gelu(u):
    inner = u * (0.7978845608028654 + 0.035677408136300125 * (u * u))
    half = 0.5 * u
    return half + half * jnp.tanh(inner)


def block_kernel(dims, x_hbm, w1_hbm, w2_hbm, kp_hbm, vp_hbm, wmod_hbm, cond, bmod, b1_in, b2_in, pos, freqs, gains,
                 xo_hbm, kn_hbm, vn_hbm,
                 w1, w2s, kbuf, vt, sbufs, tops, parts, acts, qrhs, h, xs, snd, acc, attn, vst, modp, b1, gtab,
                 w1_sem, wm_sem, w2s_sem, kp_sem, vp_sem, x_sem, snd_sem, xo_sem, kn_sem, vn_sem, mod_sem, credit):
    stages, patches, tok, width, mlp, hd, axes = dims
    seq = patches * tok
    pair = 2 * hd
    pairs = width // pair
    qkv = 3 * width
    mcol = mlp // pairs
    group = 3
    bodies = pairs // group
    span = group * mcol
    per = patches // stages
    expc = LOG2E / math.sqrt(hd)
    stage = lax.axis_index('pp') if stages > 1 else jnp.int32(0)
    last = stages - 1

    def w1_copy(j):
        cols = pl.ds(j * (qkv // 3), qkv // 3)
        return pltpu.make_async_copy(w1_hbm.at[:, cols], w1.at[:, cols], w1_sem.at[j])

    def wm_copy(j):
        if isinstance(j, int):
            lo = 0 if j == 0 else j * span + mcol
            cols = pl.ds(qkv + lo, min((j + 1) * span + mcol, mlp) - lo)
        else:
            cols = pl.ds(pl.multiple_of(qkv + j * span + mcol, mcol), span)
        return pltpu.make_async_copy(w1_hbm.at[:, cols], w1.at[:, cols], wm_sem.at[j])

    def w2_copy(par, j):
        row = j * span + width if j < bodies else 0
        return pltpu.make_async_copy(w2_hbm.at[pl.ds(row, span), :], w2s.at[par], w2s_sem.at[par])

    def w2_next(par, j):
        row = pl.multiple_of(j * span + width, mcol)
        return pltpu.make_async_copy(w2_hbm.at[pl.ds(row, span), :], w2s.at[par], w2s_sem.at[par])

    kp_copy = pltpu.make_async_copy(kp_hbm.at[pl.ds(tok, seq - tok), :], kbuf.at[pl.ds(tok, seq - tok), :], kp_sem)

    vrows = mcol
    vparts = seq // vrows

    def vp_part(p):
        return divmod(p * vrows, span)

    def vp_copy(p):
        par, row = vp_part(p)
        return pltpu.make_async_copy(vp_hbm.at[pl.ds(p * vrows, vrows), :], w2s.at[par, pl.ds(row, vrows), :], vp_sem.at[p])

    def x_copy(m, slot):
        return pltpu.make_async_copy(x_hbm.at[m], xs.at[slot], x_sem.at[slot])

    def mod_copy(c):
        cols = pl.ds(c * width, width)
        return pltpu.make_async_copy(wmod_hbm.at[:, cols], w1.at[:, pl.ds(qkv + c * width, width)], mod_sem.at[c])

    def kn_copy(m):
        rows = pl.ds(pl.multiple_of(m * tok, tok), tok)
        return pltpu.make_async_copy(kbuf.at[rows, :], kn_hbm.at[rows, :], kn_sem)

    def vn_copy(m):
        rows = pl.ds(pl.multiple_of(m * tok, tok), tok)
        return pltpu.make_async_copy(vst, vn_hbm.at[rows, :], vn_sem)

    def send_copy(slot):
        return pltpu.make_async_remote_copy(
            src_ref=snd, dst_ref=xs.at[slot], send_sem=snd_sem, recv_sem=x_sem.at[slot],
            device_id={'pp': jnp.minimum(stage + 1, last)}, device_id_type=MESH)

    def give_copy(owner, place):
        return pltpu.make_async_remote_copy(
            src_ref=snd, dst_ref=xo_hbm.at[place], send_sem=snd_sem, recv_sem=xo_sem.at[place],
            device_id={'pp': owner}, device_id_type=MESH)

    def keep_copy(place):
        return pltpu.make_async_copy(snd, xo_hbm.at[place], snd_sem)

    if stages > 1:
        barrier = pltpu.get_barrier_semaphore()

        def greet(d, c):
            pl.semaphore_signal(barrier, inc=1, device_id={'pp': lax.rem(stage + d, stages)}, device_id_type=MESH)
            return c
        lax.fori_loop(1, stages, greet, 0)

    @pl.when(stage == 0)
    def _():
        x_copy(0, 0).start()
        x_copy(1, 1).start()
    for c in range(3):
        mod_copy(c).start()
    for j in range(3):
        w1_copy(j).start()
    for p in range(vparts):
        vp_copy(p).start()
    kp_copy.start()

    qrhs[...] = jnp.zeros_like(qrhs)
    b1[...] = b1_in[...].astype(F32)

    odd_row = (lax.broadcasted_iota(jnp.int32, (hd, tok), 0) % 2) == 1

    def swap(v):
        v3 = v.reshape(hd // 8, 8, tok)
        return jnp.where(odd_row, pltpu.roll(v3, 1, 1).reshape(hd, tok), pltpu.roll(v3, 7, 1).reshape(hd, tok))

    def twice(v):
        return jnp.broadcast_to(v[:, None, :], (hd // 2, 2, tok)).reshape(hd, tok)

    for i in range(2):
        g = jnp.broadcast_to(gains[i:i + 1, :].astype(F32), (tok, hd)).T
        gtab[2 * i] = g
        gtab[2 * i + 1] = swap(g)
    modp[3:4, :] = b2_in[...].astype(F32)
    c32 = cond[...].astype(F32)
    act_c = (c32 * (1.0 / (1.0 + jnp.exp(-c32)))).astype(BF16)
    for c in range(3):
        mod_copy(c).wait()
        for n in range(width // mcol):
            lo = c * width + n * mcol
            v = mm(act_c, w1[:, qkv + lo:qkv + lo + mcol]) + bmod[:, lo:lo + mcol].astype(F32)
            modp[c:c + 1, n * mcol:(n + 1) * mcol] = v + 1.0 if c == 1 else v
    wm_copy(0).start()
    for p in range(vparts):
        vp_copy(p).wait()
        par, row = vp_part(p)

        def turn(d, c, p=p, par=par, row=row):
            ds = pl.ds(pl.multiple_of(d * pair, pair), pair)
            for t in range(vrows // tok):
                if p * vrows + t * tok >= tok:
                    vt[ds, pl.ds(p * vrows + t * tok, tok)] = w2s[par, pl.ds(row + t * tok, tok), ds].T
            return c
        lax.fori_loop(0, pairs, turn, 0, unroll=2)
    w2_copy(0, 0).start()
    for j in range(1, bodies):
        wm_copy(j).start()
    kp_copy.wait()
    for j in range(3):
        w1_copy(j).wait()
    wm_copy(0).wait()

    if stages > 1:
        pl.semaphore_wait(barrier, stages - 1)

    def patch_step(m, carry):
        slot = lax.rem(m, 2)
        rows = pl.ds(pl.multiple_of(m * tok, tok), tok)
        x_copy(0, slot).wait()
        @pl.when(m >= 1)
        def _():
            vn_copy(0).wait()
            kn_copy(0).wait()

        w2_copy(lax.rem(m + 1, 2), 1).start()

        xv = xs[slot].astype(F32)
        cen = xv - jnp.mean(xv, axis=1, keepdims=True)
        nrm = cen * lax.rsqrt(jnp.mean(cen * cen, axis=1, keepdims=True) + 1e-6)
        h[...] = (nrm * modp[1:2, :] + modp[0:1, :]).astype(BF16)
        acc[...] = jnp.zeros_like(acc)

        angle = jnp.concatenate([freqs[lo:hi, :] * pos[axis, pl.ds(m, 1), :].astype(F32) for axis, (lo, hi) in enumerate(axes)], axis=0)
        cos_t = twice(jnp.cos(angle))
        sin_t = twice(jnp.sin(angle))
        sin_t = jnp.where(odd_row, sin_t, -sin_t)
        tab_q = (cos_t * gtab[0], sin_t * gtab[1])
        tab_k = (cos_t * gtab[2], sin_t * gtab[3])
        blk = 2 * pair

        def head_norm(raw, tabs):
            raw_t = raw.T.astype(F32)
            heads = []
            for r in range(2):
                part = raw_t[r * hd:(r + 1) * hd, :]
                ssq = jnp.sum(part * part, axis=0, keepdims=True)
                inv = lax.rsqrt(ssq * (1.0 / hd) + 1e-6)
                heads.append((part * tabs[0] + swap(part) * tabs[1]) * inv)
            return jnp.concatenate(heads, axis=0)

        wide = 2 * blk

        def proj(base, j):
            cols = slice(base + j * wide, base + (j + 1) * wide)
            return (mm(h[...], w1[:, cols]) + b1[:, cols]).astype(BF16)

        def put_q(raw, j):
            for t in range(4):
                n = 4 * j + t
                q32 = head_norm(raw[:, t * pair:(t + 1) * pair], tab_q).astype(BF16).astype(F32) * expc
                hi = q32.astype(BF16)
                lo = (q32 - hi.astype(F32)).astype(BF16)
                for r, qt in ((0, hi), (pair, lo)):
                    qrhs[n, r:r + hd, 0:tok] = qt[0:hd, :]
                    qrhs[n, r + hd:r + pair, tok:2 * tok] = qt[hd:pair, :]

        def put_k(raw, j):
            for t in range(4):
                n = 4 * j + t
                kbuf[rows, n * pair:(n + 1) * pair] = head_norm(raw[:, t * pair:(t + 1) * pair], tab_k).astype(BF16).T

        def put_v(raw, j):
            vst[:, j * wide:(j + 1) * wide] = raw
            vt[j * wide:(j + 1) * wide, rows] = raw.T

        ck = 2 * tok
        nck = seq // ck
        ring = 12
        lead = nck + 1

        def score(i, b, place):
            lanes = pl.ds(pl.multiple_of(i * pair, pair), pair)
            found = []
            for r in range(2):
                kc = kbuf[b * ck + r * tok:b * ck + (r + 1) * tok, lanes]
                v = mm(jnp.concatenate([kc, kc], axis=1), qrhs[i])
                sbufs[place, r * tok:(r + 1) * tok, :] = v
                found.append(jnp.max(v.reshape(tok // 8, 8, 2 * tok), axis=0))
            return jnp.maximum(found[0], found[1])

        def high(tops8):
            t8 = functools.reduce(jnp.maximum, tops8)
            return jnp.max(t8, axis=0, keepdims=True)

        work = []
        for j in range(width // wide):
            work += [(put_q, 0, j), (put_k, width, j)]
        work += [(put_v, 2 * width, j) for j in range(width // wide)]
        held = None
        for put, base, j in work:
            raw = proj(base, j)
            if held is not None:
                held[0](held[1], held[2])
            held = (put, raw, j)
            if put is put_v and j == 0:
                w2_copy(lax.rem(m, 2), 0).wait()
                tops8 = [score(0, b, b) for b in range(nck)]
                tops8.append(score(1, 0, nck))
        steps = group * nck
        kp = width // ck

        def plan(final):
            places = {}
            for p in range(group):
                if not final or p < group - 1:
                    for k in range(kp):
                        places.setdefault(nck * p + UPS[k], []).append(('up', p, k))
                for k in range(kp // 2):
                    if final:
                        at = LASTS[p * 3 + k]
                    else:
                        at = DOWNS[p * 3 + k]
                    places.setdefault(at, []).append(('down', p, k))
            return places

        def up_piece(n, k):
            ks = slice(k * ck, (k + 1) * ck)
            return mm(h[:, ks], w1[ks, pl.ds(pl.multiple_of(qkv + n * mcol, mcol), mcol)])

        def activate(ups, n):
            up = (functools.reduce(jnp.add, ups) + b1[:, pl.ds(pl.multiple_of(qkv + n * mcol, mcol), mcol)]).astype(BF16)
            return gelu(up.astype(F32)).astype(BF16)

        def body(j, final, top, part, act0):
            par = lax.rem(m + j, 2)
            tops8 = [None] * nck + [part]
            places = plan(final)
            ups = []
            act = {0: act0}
            probs = None
            tots = []
            outs = []
            nexttop = None
            for t in range(steps + 1):
                u, b = divmod(t, nck)
                new = None
                if t < steps:
                    if b == 0 and u > 0:
                        top = nexttop
                    e = jnp.exp2(sbufs[t % ring] - top)
                    tots.append(jnp.sum(e.reshape(ck // 8, 8, 2 * tok), axis=0))
                    new = e.astype(BF16)
                    q = t + lead
                    if q < steps or not final:
                        tops8.append(score(group * j + q // nck, q % nck, q % ring))
                        if b == nck - 2:
                            nexttop = high(tops8[(u + 1) * nck:(u + 2) * nck])
                if t > 0:
                    pu, pb = divmod(t - 1, nck)
                    lanes = pl.ds(pl.multiple_of((group * j + pu) * pair, pair), pair)
                    outs.append(mm(vt[lanes, pb * ck:(pb + 1) * ck], probs))
                    if pb == nck - 1:
                        inv = 1.0 / jnp.sum(functools.reduce(jnp.add, tots[:nck]), axis=0, keepdims=True)
                        both = 0
                        for r in range(2):
                            out = functools.reduce(jnp.add, outs[r::2])
                            both = both + jnp.concatenate([out[0:hd, 0:tok] * inv[:, 0:tok], out[hd:pair, tok:2 * tok] * inv[:, tok:2 * tok]], axis=0)
                        attn[:, lanes] = both.astype(BF16).T
                        outs = []
                        tots = tots[nck:]
                probs = new
                for kind, p, k in places.get(t, ()):
                    if kind == 'up':
                        ups.append(up_piece(group * j + p + 1, k))
                        if k == kp - 1:
                            act[p + 1] = activate(ups, group * j + p + 1)
                            ups = []
                    else:
                        ks = slice(k * mcol, (k + 1) * mcol)
                        acc[:, ks] += mm(act[p], w2s[par, p * mcol:(p + 1) * mcol, ks])
            if not final:
                tops[...] = nexttop
                parts[...] = tops8[-1]
                acts[...] = act[group]

        act0 = activate([up_piece(0, k) for k in range(kp)], 0)
        held[0](held[1], held[2])
        body(0, False, high(tops8[:nck]), tops8[nck], act0)

        def start(j):
            @pl.when(m == 0)
            def _():
                wm_copy(j).wait()
            w2_copy(lax.rem(m + j, 2), 0).wait()

        def body_step(j, c):
            start(j)
            w2_next(lax.rem(m + j + 1, 2), j + 1).start()
            body(j, False, tops[...], parts[...], acts[...])
            return c
        lax.fori_loop(1, bodies - 1, body_step, 0)
        @pl.when(m >= 1)
        def _():
            if stages > 1:
                @pl.when(stage < last)
                def _():
                    send_copy(slot).wait_send()

                @pl.when(stage == last)
                def _():
                    keep_copy(0).wait()
            else:
                keep_copy(0).wait()

        if stages > 1:
            @pl.when(jnp.logical_and(stage < last, m >= 2))
            def _():
                pl.semaphore_wait(credit, 1)

        start(bodies - 1)
        w2_copy(lax.rem(m + bodies, 2), bodies).start()
        kn_copy(m).start()
        vn_copy(m).start()
        body(bodies - 1, True, tops[...], parts[...], acts[...])

        w2par = lax.rem(m + bodies, 2)
        w2_copy(w2par, 0).wait()

        w2_copy(1 - w2par, 0).start()

        sums = []
        cut = (pairs - 2) * pair
        for n in range(width // wide):
            cols = slice(n * wide, (n + 1) * wide)
            sums.append(mm(attn[:, 0:cut], w2s[w2par, 0:cut, cols]))
        for n in range(width // wide):
            cols = slice(n * wide, (n + 1) * wide)
            o = sums[n] + mm(attn[:, cut:width], w2s[w2par, cut:width, cols]) + acc[:, cols] + modp[3:4, cols]
            snd[:, cols] = (xs[slot, :, cols].astype(F32) + modp[2:3, cols] * o).astype(BF16)

        if stages > 1:
            @pl.when(stage < last)
            def _():
                send_copy(slot).start()

            @pl.when(stage == last)
            def _():
                owner = m // per

                @pl.when(owner < last)
                def _():
                    give_copy(jnp.minimum(owner, last - 1), lax.rem(m, per)).start()

                @pl.when(owner == last)
                def _():
                    keep_copy(lax.rem(m, per)).start()

            @pl.when(jnp.logical_and(stage > 0, m + 2 < patches))
            def _():
                pl.semaphore_signal(credit, inc=1, device_id={'pp': jnp.maximum(stage - 1, 0)}, device_id_type=MESH)
        else:
            keep_copy(m).start()

        @pl.when(jnp.logical_and(stage == 0, m + 2 < patches))
        def _():
            x_copy(m + 2, slot).start()
        return carry

    lax.fori_loop(0, patches, patch_step, 0)

    kn_copy(0).wait()
    vn_copy(0).wait()
    w2_copy(patches % 2, 0).wait()
    if stages > 1:
        @pl.when(stage < last)
        def _():
            send_copy(0).wait_send()
            for place in range(per):
                give_copy(0, place).wait_recv()

        @pl.when(stage == last)
        def _():
            keep_copy(0).wait()
    else:
        keep_copy(0).wait()


def rope_freqs(head_dim, lanes):
    axis_zero = head_dim // 8
    axis_rest = (head_dim - axis_zero) // 2
    rows = []
    axes = []
    for dim in (axis_zero, axis_rest, head_dim - axis_zero - axis_rest):
        axes.append((len(rows), len(rows) + dim // 2))
        rows += [1.0 / 10000.0 ** (i / dim) for i in range(0, dim, 2)]
    return np.broadcast_to(np.asarray(rows, np.float32)[:, None], (len(rows), lanes)), tuple(axes)


def make_stage(stages):
    def stage_program(x_in, cond_vec, pos_ids, w_mod, b_mod, w_one, b_one, qk_scale, w_two, b_two, k_prev, v_prev):
        batch, patches, tok, width = x_in.shape
        hd = qk_scale.shape[-1]
        mlp = w_two.shape[1] - width
        seq = patches * tok
        pair = 2 * hd
        pairs = width // pair
        mcol = mlp // pairs
        per = patches // stages
        freqs, axes = rope_freqs(hd, tok)
        hbm = functools.partial(pltpu.with_memory_space_constraint, memory_space=pltpu.HBM)
        dims = (stages, patches, tok, width, mlp, hd, axes)
        out_patches = per
        x_out, k_new, v_new = pl.pallas_call(
            functools.partial(block_kernel, dims),
            out_shape=(jax.ShapeDtypeStruct((out_patches, tok, width), BF16),
                       jax.ShapeDtypeStruct((seq, width), BF16), jax.ShapeDtypeStruct((seq, width), BF16)),
            in_specs=[pl.BlockSpec(memory_space=pltpu.HBM)] * 6 + [pl.BlockSpec(memory_space=pltpu.VMEM)] * 7,
            out_specs=(pl.BlockSpec(memory_space=pltpu.HBM),) * 3,
            scratch_shapes=[
                pltpu.VMEM((width, 3 * width + mlp), BF16),
                pltpu.VMEM((2, 3 * mcol, width), BF16),
                pltpu.VMEM((seq, width), BF16),
                pltpu.VMEM((width, seq), BF16),
                pltpu.VMEM((12, 2 * tok, 2 * tok), F32),
                pltpu.VMEM((1, 2 * tok), F32),
                pltpu.VMEM((8, 2 * tok), F32),
                pltpu.VMEM((tok, mcol), BF16),
                pltpu.VMEM((pairs, 2 * pair, 2 * tok), BF16),
                pltpu.VMEM((tok, width), BF16),
                pltpu.VMEM((2, tok, width), BF16),
                pltpu.VMEM((tok, width), BF16),
                pltpu.VMEM((tok, width), F32),
                pltpu.VMEM((tok, width), BF16),
                pltpu.VMEM((tok, width), BF16),
                pltpu.VMEM((4, width), F32),
                pltpu.VMEM((1, 3 * width + mlp), F32),
                pltpu.VMEM((4, hd, tok), F32),
                pltpu.SemaphoreType.DMA((3,)),
                pltpu.SemaphoreType.DMA((pairs // 3,)),
                pltpu.SemaphoreType.DMA((2,)),
                pltpu.SemaphoreType.DMA,
                pltpu.SemaphoreType.DMA((4,)),
                pltpu.SemaphoreType.DMA((2,)),
                pltpu.SemaphoreType.DMA,
                pltpu.SemaphoreType.DMA((per,)),
                pltpu.SemaphoreType.DMA,
                pltpu.SemaphoreType.DMA,
                pltpu.SemaphoreType.DMA((3,)),
                pltpu.SemaphoreType.REGULAR,
            ],
            compiler_params=pltpu.CompilerParams(
                vmem_limit_bytes=67043328, **(dict(collective_id=0, has_side_effects=True) if stages > 1 else {})),
            name='blocks',
        )(hbm(x_in[0]), hbm(w_one[0]), hbm(w_two[0]), hbm(k_prev.reshape(seq, width)), hbm(v_prev.reshape(seq, width)),
          hbm(w_mod[0]), cond_vec, b_mod, b_one, b_two, pos_ids.transpose(2, 0, 1), freqs, qk_scale[0])
        return x_out[None], k_new.reshape(k_prev.shape), v_new.reshape(v_prev.shape)
    return stage_program


def solution(mesh):
    stages = mesh.shape['pp']
    return jax.shard_map(
        make_stage(stages), mesh=mesh,
        in_specs=(P('dp'), P('dp'), P(), P('pp'), P('pp'), P('pp'), P('pp'), P('pp'), P('pp'), P('pp'), P('pp', 'dp'), P('pp', 'dp')),
        out_specs=(P('dp', 'pp'), P('pp', 'dp'), P('pp', 'dp')),
        check_vma=False)
```

```python
import functools
import math

import jax
import jax.numpy as jnp
import numpy as np
from jax import lax
from jax.experimental import pallas as pl
from jax.experimental.pallas import tpu as pltpu
from jax.sharding import PartitionSpec as P

MESH = pl.DeviceIdType.MESH
F32 = jnp.float32
BF16 = jnp.bfloat16
LOG2E = 1.4426950408889634


DOWNS = (0, 1, 4, 8, 9, 12, 16, 17, 20)
LASTS = (2, 4, 6, 16, 17, 18, 20, 21, 22)
UPS = (2, 3, 4, 5, 6, 7)


def mm(a, b):
    return jnp.dot(a, b, preferred_element_type=F32)


def gelu(u):
    inner = u * (0.7978845608028654 + 0.035677408136300125 * (u * u))
    half = 0.5 * u
    return half + half * jnp.tanh(inner)


def block_kernel(dims, x_hbm, w1_hbm, w2_hbm, kp_hbm, vp_hbm, wmod_hbm, cond, bmod, b1_in, b2_in, pos, gains,
                 xo_hbm, kn_hbm, vn_hbm,
                 w1, w2s, kbuf, vt, sbufs, tops, parts, acts, qrhs, h, xs, snd, acc, attn, vst, modp, b1, gtab, freqs,
                 w1_sem, wm_sem, w2s_sem, kp_sem, vp_sem, x_sem, snd_sem, xo_sem, kn_sem, vn_sem, mod_sem, credit):
    stages, patches, tok, width, mlp, hd = dims
    seq = patches * tok
    pair = 2 * hd
    pairs = width // pair
    qkv = 3 * width
    mcol = mlp // pairs
    group = 3
    bodies = pairs // group
    span = group * mcol
    per = patches // stages
    expc = LOG2E / math.sqrt(hd)
    stage = lax.axis_index('pp') if stages > 1 else jnp.int32(0)
    last = stages - 1

    def w1_copy(j):
        cols = pl.ds(j * (qkv // 3), qkv // 3)
        return pltpu.make_async_copy(w1_hbm.at[:, cols], w1.at[:, cols], w1_sem.at[j])

    def wm_copy(j):
        if isinstance(j, int):
            lo = 0 if j == 0 else j * span + mcol
            cols = pl.ds(qkv + lo, min((j + 1) * span + mcol, mlp) - lo)
        else:
            cols = pl.ds(pl.multiple_of(qkv + j * span + mcol, mcol), span)
        return pltpu.make_async_copy(w1_hbm.at[:, cols], w1.at[:, cols], wm_sem.at[j])

    def w2_copy(par, j):
        row = j * span + width if j < bodies else 0
        return pltpu.make_async_copy(w2_hbm.at[pl.ds(row, span), :], w2s.at[par], w2s_sem.at[par])

    def w2_next(par, j):
        row = pl.multiple_of(j * span + width, mcol)
        return pltpu.make_async_copy(w2_hbm.at[pl.ds(row, span), :], w2s.at[par], w2s_sem.at[par])

    kp_copy = pltpu.make_async_copy(kp_hbm.at[pl.ds(tok, seq - tok), :], kbuf.at[pl.ds(tok, seq - tok), :], kp_sem)

    vrows = mcol
    vparts = seq // vrows

    def vp_part(p):
        return divmod(p * vrows, span)

    def vp_copy(p):
        par, row = vp_part(p)
        return pltpu.make_async_copy(vp_hbm.at[pl.ds(p * vrows, vrows), :], w2s.at[par, pl.ds(row, vrows), :], vp_sem.at[p])

    def x_copy(m, slot):
        return pltpu.make_async_copy(x_hbm.at[m], xs.at[slot], x_sem.at[slot])

    def mod_copy(c):
        cols = pl.ds(c * width, width)
        return pltpu.make_async_copy(wmod_hbm.at[:, cols], w1.at[:, pl.ds(qkv + c * width, width)], mod_sem.at[c])

    def kn_copy(m):
        rows = pl.ds(pl.multiple_of(m * tok, tok), tok)
        return pltpu.make_async_copy(kbuf.at[rows, :], kn_hbm.at[rows, :], kn_sem)

    def vn_copy(m):
        rows = pl.ds(pl.multiple_of(m * tok, tok), tok)
        return pltpu.make_async_copy(vst, vn_hbm.at[rows, :], vn_sem)

    def send_copy(slot, cols=pl.ds(0, width)):
        return pltpu.make_async_remote_copy(
            src_ref=snd.at[:, cols], dst_ref=xs.at[slot, :, cols], send_sem=snd_sem, recv_sem=x_sem.at[slot],
            device_id={'pp': jnp.minimum(stage + 1, last)}, device_id_type=MESH)

    def give_copy(owner, place):
        return pltpu.make_async_remote_copy(
            src_ref=snd, dst_ref=xo_hbm.at[place], send_sem=snd_sem, recv_sem=xo_sem.at[place],
            device_id={'pp': owner}, device_id_type=MESH)

    def keep_copy(place):
        return pltpu.make_async_copy(snd, xo_hbm.at[place], snd_sem)

    if stages > 1:
        barrier = pltpu.get_barrier_semaphore()

        def greet(d, c):
            pl.semaphore_signal(barrier, inc=1, device_id={'pp': lax.rem(stage + d, stages)}, device_id_type=MESH)
            return c
        lax.fori_loop(1, stages, greet, 0)

    @pl.when(stage == 0)
    def _():
        x_copy(0, 0).start()
        x_copy(1, 1).start()
    for c in range(3):
        mod_copy(c).start()
    for p in range(vparts):
        vp_copy(p).start()
    for j in range(3):
        w1_copy(j).start()
    kp_copy.start()

    qrhs[...] = jnp.zeros_like(qrhs)
    b1[...] = b1_in[...].astype(F32)

    freq_rows, axes = rope_rows(hd)
    row8 = lax.broadcasted_iota(jnp.int32, (8, tok), 0)
    for g in range(hd // 16):
        part = jnp.zeros((8, tok), F32)
        for r in range(8):
            part = jnp.where(row8 == r, freq_rows[8 * g + r], part)
        freqs[8 * g:8 * g + 8, :] = part
    odd_row = (lax.broadcasted_iota(jnp.int32, (hd, tok), 0) % 2) == 1

    def swap(v):
        v3 = v.reshape(hd // 8, 8, tok)
        return jnp.where(odd_row, pltpu.roll(v3, 1, 1).reshape(hd, tok), pltpu.roll(v3, 7, 1).reshape(hd, tok))

    def twice(v):
        return jnp.broadcast_to(v[:, None, :], (hd // 2, 2, tok)).reshape(hd, tok)

    for i in range(2):
        g = jnp.broadcast_to(gains[i:i + 1, :].astype(F32), (tok, hd)).T
        gtab[2 * i] = g
        gtab[2 * i + 1] = swap(g)
    modp[3:4, :] = b2_in[...].astype(F32)
    c32 = cond[...].astype(F32)
    act_c = (c32 * (1.0 / (1.0 + jnp.exp(-c32)))).astype(BF16)
    for c in range(3):
        mod_copy(c).wait()
        for n in range(width // mcol):
            lo = c * width + n * mcol
            v = mm(act_c, w1[:, qkv + lo:qkv + lo + mcol]) + bmod[:, lo:lo + mcol].astype(F32)
            modp[c:c + 1, n * mcol:(n + 1) * mcol] = v + 1.0 if c == 1 else v
    wm_copy(0).start()
    for p in range(vparts):
        vp_copy(p).wait()
        par, row = vp_part(p)

        def turn(d, c, p=p, par=par, row=row):
            ds = pl.ds(pl.multiple_of(d * pair, pair), pair)
            for t in range(vrows // tok):
                if p * vrows + t * tok >= tok:
                    vt[ds, pl.ds(p * vrows + t * tok, tok)] = w2s[par, pl.ds(row + t * tok, tok), ds].T
            return c
        lax.fori_loop(0, pairs, turn, 0, unroll=2)
    w2_copy(0, 0).start()
    wm_copy(1).start()
    for j in range(3):
        w1_copy(j).wait()

    if stages > 1:
        pl.semaphore_wait(barrier, stages - 1)

    def patch_step(m, carry):
        slot = lax.rem(m, 2)
        rows = pl.ds(pl.multiple_of(m * tok, tok), tok)
        x_copy(0, slot).wait()
        @pl.when(m >= 1)
        def _():
            vn_copy(0).wait()
            kn_copy(0).wait()

        w2_copy(lax.rem(m + 1, 2), 1).start()

        @pl.when(m == 0)
        def _():
            for j in range(2, bodies):
                wm_copy(j).start()

        xv = xs[slot].astype(F32)
        cen = xv - jnp.mean(xv, axis=1, keepdims=True)
        nrm = cen * lax.rsqrt(jnp.mean(cen * cen, axis=1, keepdims=True) + 1e-6)
        h[...] = (nrm * modp[1:2, :] + modp[0:1, :]).astype(BF16)
        acc[...] = jnp.zeros_like(acc)

        angle = jnp.concatenate([freqs[lo:hi, :] * pos[axis, pl.ds(m, 1), :].astype(F32) for axis, (lo, hi) in enumerate(axes)], axis=0)
        cos_t = twice(jnp.cos(angle))
        sin_t = twice(jnp.sin(angle))
        sin_t = jnp.where(odd_row, sin_t, -sin_t)
        tab_q = (cos_t * gtab[0], sin_t * gtab[1])
        tab_k = (cos_t * gtab[2], sin_t * gtab[3])
        blk = 2 * pair

        def head_norm(raw, tabs):
            raw_t = raw.T.astype(F32)
            heads = []
            for r in range(2):
                part = raw_t[r * hd:(r + 1) * hd, :]
                ssq = jnp.sum(part * part, axis=0, keepdims=True)
                inv = lax.rsqrt(ssq * (1.0 / hd) + 1e-6)
                heads.append((part * tabs[0] + swap(part) * tabs[1]) * inv)
            return jnp.concatenate(heads, axis=0)

        wide = 2 * blk

        def proj(base, j):
            cols = slice(base + j * wide, base + (j + 1) * wide)
            return (mm(h[...], w1[:, cols]) + b1[:, cols]).astype(BF16)

        def put_q(raw, j):
            for t in range(4):
                n = 4 * j + t
                q32 = head_norm(raw[:, t * pair:(t + 1) * pair], tab_q).astype(BF16).astype(F32) * expc
                hi = q32.astype(BF16)
                lo = (q32 - hi.astype(F32)).astype(BF16)
                for r, qt in ((0, hi), (pair, lo)):
                    qrhs[n, r:r + hd, 0:tok] = qt[0:hd, :]
                    qrhs[n, r + hd:r + pair, tok:2 * tok] = qt[hd:pair, :]

        def put_k(raw, j):
            for t in range(4):
                n = 4 * j + t
                kbuf[rows, n * pair:(n + 1) * pair] = head_norm(raw[:, t * pair:(t + 1) * pair], tab_k).astype(BF16).T

        def put_v(raw, j):
            vst[:, j * wide:(j + 1) * wide] = raw
            vt[j * wide:(j + 1) * wide, rows] = raw.T

        ck = 2 * tok
        nck = seq // ck
        ring = 12
        lead = nck + 1

        def score(i, b, place):
            lanes = pl.ds(pl.multiple_of(i * pair, pair), pair)
            found = []
            for r in range(2):
                kc = kbuf[b * ck + r * tok:b * ck + (r + 1) * tok, lanes]
                v = mm(jnp.concatenate([kc, kc], axis=1), qrhs[i])
                sbufs[place, r * tok:(r + 1) * tok, :] = v
                found.append(jnp.max(v.reshape(tok // 8, 8, 2 * tok), axis=0))
            return jnp.maximum(found[0], found[1])

        def high(tops8):
            t8 = functools.reduce(jnp.maximum, tops8)
            return jnp.max(t8, axis=0, keepdims=True)

        work = []
        for j in range(width // wide):
            work += [(put_q, 0, j), (put_k, width, j)]
        work += [(put_v, 2 * width, j) for j in range(width // wide)]
        held = None
        for put, base, j in work:
            raw = proj(base, j)
            if held is not None:
                held[0](held[1], held[2])
            held = (put, raw, j)
            if put is put_v and j == 0:
                w2_copy(lax.rem(m, 2), 0).wait()

                @pl.when(m == 0)
                def _():
                    kp_copy.wait()
                    wm_copy(0).wait()
                tops8 = [score(0, b, b) for b in range(nck)]
                tops8.append(score(1, 0, nck))
        steps = group * nck
        kp = width // ck

        def plan(final):
            places = {}
            for p in range(group):
                if not final or p < group - 1:
                    for k in range(kp):
                        places.setdefault(nck * p + UPS[k], []).append(('up', p, k))
                for k in range(kp // 2):
                    if final:
                        at = LASTS[p * 3 + k]
                    else:
                        at = DOWNS[p * 3 + k]
                    places.setdefault(at, []).append(('down', p, k))
            return places

        def up_piece(n, k):
            ks = slice(k * ck, (k + 1) * ck)
            return mm(h[:, ks], w1[ks, pl.ds(pl.multiple_of(qkv + n * mcol, mcol), mcol)])

        def activate(ups, n):
            up = (functools.reduce(jnp.add, ups) + b1[:, pl.ds(pl.multiple_of(qkv + n * mcol, mcol), mcol)]).astype(BF16)
            return gelu(up.astype(F32)).astype(BF16)

        def body(j, final, top, part, act0):
            par = lax.rem(m + j, 2)
            tops8 = [None] * nck + [part]
            places = plan(final)
            ups = []
            act = {0: act0}
            probs = None
            tots = []
            outs = []
            nexttop = None
            for t in range(steps + 1):
                u, b = divmod(t, nck)
                new = None
                if t < steps:
                    if b == 0 and u > 0:
                        top = nexttop
                    e = jnp.exp2(sbufs[t % ring] - top)
                    tots.append(jnp.sum(e.reshape(ck // 8, 8, 2 * tok), axis=0))
                    new = e.astype(BF16)
                    q = t + lead
                    if q < steps or not final:
                        tops8.append(score(group * j + q // nck, q % nck, q % ring))
                        if b == nck - 2:
                            nexttop = high(tops8[(u + 1) * nck:(u + 2) * nck])
                if t > 0:
                    pu, pb = divmod(t - 1, nck)
                    lanes = pl.ds(pl.multiple_of((group * j + pu) * pair, pair), pair)
                    outs.append(mm(vt[lanes, pb * ck:(pb + 1) * ck], probs))
                    if pb == nck - 1:
                        inv = 1.0 / jnp.sum(functools.reduce(jnp.add, tots[:nck]), axis=0, keepdims=True)
                        both = 0
                        for r in range(2):
                            out = functools.reduce(jnp.add, outs[r::2])
                            both = both + jnp.concatenate([out[0:hd, 0:tok] * inv[:, 0:tok], out[hd:pair, tok:2 * tok] * inv[:, tok:2 * tok]], axis=0)
                        attn[:, lanes] = both.astype(BF16).T
                        outs = []
                        tots = tots[nck:]
                probs = new
                for kind, p, k in places.get(t, ()):
                    if kind == 'up':
                        ups.append(up_piece(group * j + p + 1, k))
                        if k == kp - 1:
                            act[p + 1] = activate(ups, group * j + p + 1)
                            ups = []
                    else:
                        ks = slice(k * mcol, (k + 1) * mcol)
                        acc[:, ks] += mm(act[p], w2s[par, p * mcol:(p + 1) * mcol, ks])
            if not final:
                tops[...] = nexttop
                parts[...] = tops8[-1]
                acts[...] = act[group]

        act0 = activate([up_piece(0, k) for k in range(kp)], 0)
        held[0](held[1], held[2])
        body(0, False, high(tops8[:nck]), tops8[nck], act0)

        def start(j):
            @pl.when(m == 0)
            def _():
                wm_copy(j).wait()
            w2_copy(lax.rem(m + j, 2), 0).wait()

        def body_step(j, c):
            start(j)
            w2_next(lax.rem(m + j + 1, 2), j + 1).start()
            body(j, False, tops[...], parts[...], acts[...])
            return c
        lax.fori_loop(1, bodies - 1, body_step, 0)
        @pl.when(m >= 1)
        def _():
            if stages > 1:
                @pl.when(stage < last)
                def _():
                    send_copy(slot).wait_send()

                @pl.when(stage == last)
                def _():
                    keep_copy(0).wait()
            else:
                keep_copy(0).wait()

        if stages > 1:
            @pl.when(jnp.logical_and(stage < last, m >= 2))
            def _():
                pl.semaphore_wait(credit, 1)

        start(bodies - 1)
        w2_copy(lax.rem(m + bodies, 2), bodies).start()
        kn_copy(m).start()
        vn_copy(m).start()
        body(bodies - 1, True, tops[...], parts[...], acts[...])

        w2par = lax.rem(m + bodies, 2)
        w2_copy(w2par, 0).wait()

        w2_copy(1 - w2par, 0).start()

        for n in range(width // wide):
            cols = slice(n * wide, (n + 1) * wide)
            o = mm(attn[...], w2s[w2par, :, cols]) + acc[:, cols] + modp[3:4, cols]
            snd[:, cols] = (xs[slot, :, cols].astype(F32) + modp[2:3, cols] * o).astype(BF16)
            if stages > 1:
                @pl.when(stage < last)
                def _():
                    send_copy(slot, pl.ds(n * wide, wide)).start()

        if stages > 1:
            @pl.when(stage == last)
            def _():
                owner = m // per

                @pl.when(owner < last)
                def _():
                    give_copy(jnp.minimum(owner, last - 1), lax.rem(m, per)).start()

                @pl.when(owner == last)
                def _():
                    keep_copy(lax.rem(m, per)).start()

            @pl.when(jnp.logical_and(stage > 0, m + 2 < patches))
            def _():
                pl.semaphore_signal(credit, inc=1, device_id={'pp': jnp.maximum(stage - 1, 0)}, device_id_type=MESH)
        else:
            keep_copy(m).start()

        @pl.when(jnp.logical_and(stage == 0, m + 2 < patches))
        def _():
            x_copy(m + 2, slot).start()
        return carry

    lax.fori_loop(0, patches, patch_step, 0)

    kn_copy(0).wait()
    vn_copy(0).wait()
    w2_copy(patches % 2, 0).wait()
    if stages > 1:
        @pl.when(stage < last)
        def _():
            send_copy(0).wait_send()
            for place in range(per):
                give_copy(0, place).wait_recv()

        @pl.when(stage == last)
        def _():
            keep_copy(0).wait()
    else:
        keep_copy(0).wait()


def rope_rows(head_dim):
    axis_zero = head_dim // 8
    axis_rest = (head_dim - axis_zero) // 2
    rows = []
    axes = []
    for dim in (axis_zero, axis_rest, head_dim - axis_zero - axis_rest):
        axes.append((len(rows), len(rows) + dim // 2))
        rows += [float(np.float32(1.0 / 10000.0 ** (i / dim))) for i in range(0, dim, 2)]
    return rows, axes


def make_stage(stages):
    def stage_program(x_in, cond_vec, pos_ids, w_mod, b_mod, w_one, b_one, qk_scale, w_two, b_two, k_prev, v_prev):
        batch, patches, tok, width = x_in.shape
        hd = qk_scale.shape[-1]
        mlp = w_two.shape[1] - width
        seq = patches * tok
        pair = 2 * hd
        pairs = width // pair
        mcol = mlp // pairs
        per = patches // stages
        hbm = functools.partial(pltpu.with_memory_space_constraint, memory_space=pltpu.HBM)
        dims = (stages, patches, tok, width, mlp, hd)
        out_patches = per
        x_out, k_new, v_new = pl.pallas_call(
            functools.partial(block_kernel, dims),
            out_shape=(jax.ShapeDtypeStruct((out_patches, tok, width), BF16),
                       jax.ShapeDtypeStruct((seq, width), BF16), jax.ShapeDtypeStruct((seq, width), BF16)),
            in_specs=[pl.BlockSpec(memory_space=pltpu.HBM)] * 6 + [pl.BlockSpec(memory_space=pltpu.VMEM)] * 6,
            out_specs=(pl.BlockSpec(memory_space=pltpu.HBM),) * 3,
            scratch_shapes=[
                pltpu.VMEM((width, 3 * width + mlp), BF16),
                pltpu.VMEM((2, 3 * mcol, width), BF16),
                pltpu.VMEM((seq, width), BF16),
                pltpu.VMEM((width, seq), BF16),
                pltpu.VMEM((12, 2 * tok, 2 * tok), F32),
                pltpu.VMEM((1, 2 * tok), F32),
                pltpu.VMEM((8, 2 * tok), F32),
                pltpu.VMEM((tok, mcol), BF16),
                pltpu.VMEM((pairs, 2 * pair, 2 * tok), BF16),
                pltpu.VMEM((tok, width), BF16),
                pltpu.VMEM((2, tok, width), BF16),
                pltpu.VMEM((tok, width), BF16),
                pltpu.VMEM((tok, width), F32),
                pltpu.VMEM((tok, width), BF16),
                pltpu.VMEM((tok, width), BF16),
                pltpu.VMEM((4, width), F32),
                pltpu.VMEM((1, 3 * width + mlp), F32),
                pltpu.VMEM((4, hd, tok), F32),
                pltpu.VMEM((hd // 2, tok), F32),
                pltpu.SemaphoreType.DMA((3,)),
                pltpu.SemaphoreType.DMA((pairs // 3,)),
                pltpu.SemaphoreType.DMA((2,)),
                pltpu.SemaphoreType.DMA,
                pltpu.SemaphoreType.DMA((4,)),
                pltpu.SemaphoreType.DMA((2,)),
                pltpu.SemaphoreType.DMA,
                pltpu.SemaphoreType.DMA((per,)),
                pltpu.SemaphoreType.DMA,
                pltpu.SemaphoreType.DMA,
                pltpu.SemaphoreType.DMA((3,)),
                pltpu.SemaphoreType.REGULAR,
            ],
            compiler_params=pltpu.CompilerParams(
                vmem_limit_bytes=67043328, **(dict(collective_id=0, has_side_effects=True) if stages > 1 else {})),
            name='blocks',
        )(hbm(x_in[0]), hbm(w_one[0]), hbm(w_two[0]), hbm(k_prev.reshape(seq, width)), hbm(v_prev.reshape(seq, width)),
          hbm(w_mod[0]), cond_vec, b_mod, b_one, b_two, pos_ids.transpose(2, 0, 1), qk_scale[0])
        return x_out[None], k_new.reshape(k_prev.shape), v_new.reshape(v_prev.shape)
    return stage_program


def solution(mesh):
    stages = mesh.shape['pp']
    return jax.shard_map(
        make_stage(stages), mesh=mesh,
        in_specs=(P('dp'), P('dp'), P(), P('pp'), P('pp'), P('pp'), P('pp'), P('pp'), P('pp'), P('pp'), P('pp', 'dp'), P('pp', 'dp')),
        out_specs=(P('dp', 'pp'), P('pp', 'dp'), P('pp', 'dp')),
        check_vma=False)
```

```python
import functools
import math

import jax
import jax.numpy as jnp
import numpy as np
from jax import lax
from jax.experimental import pallas as pl
from jax.experimental.pallas import tpu as pltpu
from jax.sharding import PartitionSpec as P

MESH = pl.DeviceIdType.MESH
F32 = jnp.float32
BF16 = jnp.bfloat16
LOG2E = 1.4426950408889634


DOWNS = (0, 1, 4, 8, 9, 12, 16, 17, 20)
LASTS = (2, 4, 6, 10, 16, 17, 19, 21, 23)
UPS = (2, 3, 4, 5, 6, 7)


QKAT = 9
UPAT = 9
WAITAT = 9
EARLY = ((0, 0, 0, 1, 1, 1), (0, 2, 4))


def mm(a, b):
    return jnp.dot(a, b, preferred_element_type=F32)


def gelu(u):
    inner = u * (0.7978845608028654 + 0.035677408136300125 * (u * u))
    half = 0.5 * u
    return half + half * jnp.tanh(inner)


def block_kernel(dims, x_hbm, w1_hbm, w2_hbm, kp_hbm, vp_hbm, wmod_hbm, cond, bmod, b1_in, b2_in, pos, gains,
                 xo_hbm, kn_hbm, vn_hbm,
                 w1, w2s, kbuf, vt, sbufs, tops, parts, acts, qrhs, h, xs, snd, acc, attn, vst, modp, b1, gtab, freqs,
                 w1_sem, wm_sem, w2s_sem, kp_sem, vp_sem, x_sem, snd_sem, xo_sem, kn_sem, vn_sem, mod_sem, credit):
    stages, patches, tok, width, mlp, hd = dims
    seq = patches * tok
    pair = 2 * hd
    pairs = width // pair
    qkv = 3 * width
    mcol = mlp // pairs
    group = 3
    bodies = pairs // group
    span = group * mcol
    per = patches // stages
    expc = LOG2E / math.sqrt(hd)
    stage = lax.axis_index('pp') if stages > 1 else jnp.int32(0)
    last = stages - 1

    def w1_copy(j):
        cols = pl.ds(j * (qkv // 3), qkv // 3)
        return pltpu.make_async_copy(w1_hbm.at[:, cols], w1.at[:, cols], w1_sem.at[j])

    def wm_copy(j):
        if isinstance(j, int):
            lo = 0 if j == 0 else j * span + mcol
            cols = pl.ds(qkv + lo, min((j + 1) * span + mcol, mlp) - lo)
        else:
            cols = pl.ds(pl.multiple_of(qkv + j * span + mcol, mcol), span)
        return pltpu.make_async_copy(w1_hbm.at[:, cols], w1.at[:, cols], wm_sem.at[j])

    def w2_copy(par, j):
        row = j * span + width if j < bodies else 0
        return pltpu.make_async_copy(w2_hbm.at[pl.ds(row, span), :], w2s.at[par], w2s_sem.at[par])

    def w2_next(par, j):
        row = pl.multiple_of(j * span + width, mcol)
        return pltpu.make_async_copy(w2_hbm.at[pl.ds(row, span), :], w2s.at[par], w2s_sem.at[par])

    kp_copy = pltpu.make_async_copy(kp_hbm.at[pl.ds(tok, seq - tok), :], kbuf.at[pl.ds(tok, seq - tok), :], kp_sem)

    vrows = mcol
    vparts = seq // vrows

    def vp_part(p):
        return divmod(p * vrows, span)

    def vp_copy(p):
        par, row = vp_part(p)
        return pltpu.make_async_copy(vp_hbm.at[pl.ds(p * vrows, vrows), :], w2s.at[par, pl.ds(row, vrows), :], vp_sem.at[p])

    def x_copy(m, slot):
        return pltpu.make_async_copy(x_hbm.at[m], xs.at[slot], x_sem.at[slot])

    def mod_copy(c):
        cols = pl.ds(c * width, width)
        return pltpu.make_async_copy(wmod_hbm.at[:, cols], w1.at[:, pl.ds(qkv + c * width, width)], mod_sem.at[c])

    def kn_copy(m):
        rows = pl.ds(pl.multiple_of(m * tok, tok), tok)
        return pltpu.make_async_copy(kbuf.at[rows, :], kn_hbm.at[rows, :], kn_sem)

    def vn_copy(m):
        rows = pl.ds(pl.multiple_of(m * tok, tok), tok)
        return pltpu.make_async_copy(vst, vn_hbm.at[rows, :], vn_sem)

    def send_copy(slot, cols=pl.ds(0, width)):
        return pltpu.make_async_remote_copy(
            src_ref=snd.at[:, cols], dst_ref=xs.at[slot, :, cols], send_sem=snd_sem, recv_sem=x_sem.at[slot],
            device_id={'pp': jnp.minimum(stage + 1, last)}, device_id_type=MESH)

    def give_copy(owner, place):
        return pltpu.make_async_remote_copy(
            src_ref=snd, dst_ref=xo_hbm.at[place], send_sem=snd_sem, recv_sem=xo_sem.at[place],
            device_id={'pp': owner}, device_id_type=MESH)

    def keep_copy(place):
        return pltpu.make_async_copy(snd, xo_hbm.at[place], snd_sem)

    if stages > 1:
        barrier = pltpu.get_barrier_semaphore()

        def greet(d, c):
            pl.semaphore_signal(barrier, inc=1, device_id={'pp': lax.rem(stage + d, stages)}, device_id_type=MESH)
            return c
        lax.fori_loop(1, stages, greet, 0)

    @pl.when(stage == 0)
    def _():
        x_copy(0, 0).start()
        x_copy(1, 1).start()
    for c in range(3):
        mod_copy(c).start()
    for p in range(vparts):
        vp_copy(p).start()
    for j in range(3):
        w1_copy(j).start()
    kp_copy.start()

    qrhs[...] = jnp.zeros_like(qrhs)
    b1[...] = b1_in[...].astype(F32)

    freq_rows, axes = rope_rows(hd)
    row8 = lax.broadcasted_iota(jnp.int32, (8, tok), 0)
    for g in range(hd // 16):
        part = jnp.zeros((8, tok), F32)
        for r in range(8):
            part = jnp.where(row8 == r, freq_rows[8 * g + r], part)
        freqs[8 * g:8 * g + 8, :] = part
    odd_row = (lax.broadcasted_iota(jnp.int32, (hd, tok), 0) % 2) == 1

    def swap(v):
        v3 = v.reshape(hd // 8, 8, tok)
        return jnp.where(odd_row, pltpu.roll(v3, 1, 1).reshape(hd, tok), pltpu.roll(v3, 7, 1).reshape(hd, tok))

    def twice(v):
        return jnp.broadcast_to(v[:, None, :], (hd // 2, 2, tok)).reshape(hd, tok)

    for i in range(2):
        g = jnp.broadcast_to(gains[i:i + 1, :].astype(F32), (tok, hd)).T
        gtab[2 * i] = g
        gtab[2 * i + 1] = swap(g)
    modp[3:4, :] = b2_in[...].astype(F32)
    c32 = cond[...].astype(F32)
    act_c = (c32 * (1.0 / (1.0 + jnp.exp(-c32)))).astype(BF16)
    for c in range(3):
        mod_copy(c).wait()
        for n in range(width // mcol):
            lo = c * width + n * mcol
            v = mm(act_c, w1[:, qkv + lo:qkv + lo + mcol]) + bmod[:, lo:lo + mcol].astype(F32)
            modp[c:c + 1, n * mcol:(n + 1) * mcol] = v + 1.0 if c == 1 else v
    for p in range(vparts):
        vp_copy(p).wait()
        par, row = vp_part(p)

        def turn(d, c, p=p, par=par, row=row):
            ds = pl.ds(pl.multiple_of(d * pair, pair), pair)
            for t in range(vrows // tok):
                if p * vrows + t * tok >= tok:
                    vt[ds, pl.ds(p * vrows + t * tok, tok)] = w2s[par, pl.ds(row + t * tok, tok), ds].T
            return c
        lax.fori_loop(0, pairs, turn, 0, unroll=2)
    w2_copy(0, 0).start()
    wm_copy(0).start()
    wm_copy(1).start()
    for j in range(3):
        w1_copy(j).wait()

    if stages > 1:
        pl.semaphore_wait(barrier, stages - 1)

    def patch_step(m, carry):
        slot = lax.rem(m, 2)
        rows = pl.ds(pl.multiple_of(m * tok, tok), tok)
        x_copy(0, slot).wait()
        @pl.when(m >= 1)
        def _():
            vn_copy(0).wait()
            kn_copy(0).wait()

        w2_copy(lax.rem(m + 1, 2), 1).start()

        @pl.when(m == 0)
        def _():
            wm_copy(2).start()

        xv = xs[slot].astype(F32)
        cen = xv - jnp.mean(xv, axis=1, keepdims=True)
        nrm = cen * lax.rsqrt(jnp.mean(cen * cen, axis=1, keepdims=True) + 1e-6)
        h[...] = (nrm * modp[1:2, :] + modp[0:1, :]).astype(BF16)
        acc[...] = jnp.zeros_like(acc)

        angle = jnp.concatenate([freqs[lo:hi, :] * pos[axis, pl.ds(m, 1), :].astype(F32) for axis, (lo, hi) in enumerate(axes)], axis=0)
        cos_t = twice(jnp.cos(angle))
        sin_t = twice(jnp.sin(angle))
        sin_t = jnp.where(odd_row, sin_t, -sin_t)
        tab_q = (cos_t * gtab[0], sin_t * gtab[1])
        tab_k = (cos_t * gtab[2], sin_t * gtab[3])
        blk = 2 * pair

        def head_norm(raw, tabs):
            raw_t = raw.T.astype(F32)
            heads = []
            for r in range(2):
                part = raw_t[r * hd:(r + 1) * hd, :]
                ssq = jnp.sum(part * part, axis=0, keepdims=True)
                inv = lax.rsqrt(ssq * (1.0 / hd) + 1e-6)
                heads.append((part * tabs[0] + swap(part) * tabs[1]) * inv)
            return jnp.concatenate(heads, axis=0)

        wide = 2 * blk

        def proj(base, j):
            cols = slice(base + j * wide, base + (j + 1) * wide)
            return (mm(h[...], w1[:, cols]) + b1[:, cols]).astype(BF16)

        def put_q(raw, j):
            for t in range(4):
                n = 4 * j + t
                q32 = head_norm(raw[:, t * pair:(t + 1) * pair], tab_q).astype(BF16).astype(F32) * expc
                hi = q32.astype(BF16)
                lo = (q32 - hi.astype(F32)).astype(BF16)
                for r, qt in ((0, hi), (pair, lo)):
                    qrhs[n, r:r + hd, 0:tok] = qt[0:hd, :]
                    qrhs[n, r + hd:r + pair, tok:2 * tok] = qt[hd:pair, :]

        def put_k(raw, j):
            for t in range(4):
                n = 4 * j + t
                kbuf[rows, n * pair:(n + 1) * pair] = head_norm(raw[:, t * pair:(t + 1) * pair], tab_k).astype(BF16).T

        def put_v(raw, j):
            vst[:, j * wide:(j + 1) * wide] = raw
            vt[j * wide:(j + 1) * wide, rows] = raw.T

        ck = 2 * tok
        nck = seq // ck
        ring = 12
        lead = nck + 1

        def score(i, b, place):
            lanes = pl.ds(pl.multiple_of(i * pair, pair), pair)
            found = []
            for r in range(2):
                kc = kbuf[b * ck + r * tok:b * ck + (r + 1) * tok, lanes]
                v = mm(jnp.concatenate([kc, kc], axis=1), qrhs[i])
                sbufs[place, r * tok:(r + 1) * tok, :] = v
                found.append(jnp.max(v.reshape(tok // 8, 8, 2 * tok), axis=0))
            return jnp.maximum(found[0], found[1])

        def high(tops8):
            t8 = functools.reduce(jnp.maximum, tops8)
            return jnp.max(t8, axis=0, keepdims=True)

        held = None
        tops8 = []
        first = [(put, base, j) for j in range(width // wide) for put, base in ((put_q, 0), (put_k, width))]
        values = [(put_v, 2 * width, j) for j in range(width // wide)]
        order = first + values
        order = order[:QKAT] + ['score'] + order[QKAT:]
        order = order[:UPAT] + ['up'] + order[UPAT:]
        order = order[:WAITAT] + ['wait'] + order[WAITAT:]
        steps = group * nck
        kp = width // ck

        def plan(j, final):
            opening = isinstance(j, int) and j == 0
            places = {}
            for p in range(group):
                if not final or p < group - 1:
                    for k in range(kp):
                        places.setdefault(EARLY[0][k] if opening and p == 0 else nck * p + UPS[k], []).append(('up', p, k))
                for k in range(kp // 2):
                    if final:
                        at = LASTS[p * 3 + k]
                    else:
                        at = EARLY[1][k] if opening and p == 0 else DOWNS[p * 3 + k]
                    places.setdefault(at, []).append(('down', p, k))
            return places

        def up_piece(n, k):
            ks = slice(k * ck, (k + 1) * ck)
            return mm(h[:, ks], w1[ks, pl.ds(pl.multiple_of(qkv + n * mcol, mcol), mcol)])

        def activate(ups, n):
            up = (functools.reduce(jnp.add, ups) + b1[:, pl.ds(pl.multiple_of(qkv + n * mcol, mcol), mcol)]).astype(BF16)
            return gelu(up.astype(F32)).astype(BF16)

        def body(j, final, top, part, act0):
            par = lax.rem(m + j, 2)
            tops8 = [None] * nck + [part]
            places = plan(j, final)
            ups = []
            act = {0: act0}
            probs = None
            tots = []
            outs = []
            nexttop = None
            for t in range(steps + 1):
                u, b = divmod(t, nck)
                new = None
                if t < steps:
                    if b == 0 and u > 0:
                        top = nexttop
                    e = jnp.exp2(sbufs[t % ring] - top)
                    tots.append(jnp.sum(e.reshape(ck // 8, 8, 2 * tok), axis=0))
                    new = e.astype(BF16)
                    q = t + lead
                    if q < steps or not final:
                        tops8.append(score(group * j + q // nck, q % nck, q % ring))
                        if b == nck - 2:
                            nexttop = high(tops8[(u + 1) * nck:(u + 2) * nck])
                if t > 0:
                    pu, pb = divmod(t - 1, nck)
                    lanes = pl.ds(pl.multiple_of((group * j + pu) * pair, pair), pair)
                    outs.append(mm(vt[lanes, pb * ck:(pb + 1) * ck], probs))
                    if pb == nck - 1:
                        inv = 1.0 / jnp.sum(functools.reduce(jnp.add, tots[:nck]), axis=0, keepdims=True)
                        both = 0
                        for r in range(2):
                            out = functools.reduce(jnp.add, outs[r::2])
                            both = both + jnp.concatenate([out[0:hd, 0:tok] * inv[:, 0:tok], out[hd:pair, tok:2 * tok] * inv[:, tok:2 * tok]], axis=0)
                        attn[:, lanes] = both.astype(BF16).T
                        outs = []
                        tots = tots[nck:]
                probs = new
                for kind, p, k in places.get(t, ()):
                    if kind == 'up':
                        ups.append(up_piece(group * j + p + 1, k))
                        if k == kp - 1:
                            act[p + 1] = activate(ups, group * j + p + 1)
                            ups = []
                    else:
                        ks = slice(k * mcol, (k + 1) * mcol)
                        acc[:, ks] += mm(act[p], w2s[par, p * mcol:(p + 1) * mcol, ks])
            if not final:
                tops[...] = nexttop
                parts[...] = tops8[-1]
                acts[...] = act[group]

        for what in order:
            if what == 'wait':
                w2_copy(lax.rem(m, 2), 0).wait()

                @pl.when(m == 0)
                def _():
                    kp_copy.wait()
                    wm_copy(0).wait()
            elif what == 'score':
                tops8 = [score(0, b, b) for b in range(nck)]
                tops8.append(score(1, 0, nck))
            elif what == 'up':
                act0 = activate([up_piece(0, k) for k in range(kp)], 0)
            else:
                put, base, j = what
                raw = proj(base, j)
                if held is not None:
                    held[0](held[1], held[2])
                held = (put, raw, j)
        held[0](held[1], held[2])
        body(0, False, high(tops8[:nck]), tops8[nck], act0)

        def start(j):
            @pl.when(m == 0)
            def _():
                wm_copy(j).wait()
            w2_copy(lax.rem(m + j, 2), 0).wait()

        def body_step(j, c):
            start(j)
            w2_next(lax.rem(m + j + 1, 2), j + 1).start()

            @pl.when(jnp.logical_and(m == 0, j == 1))
            def _():
                wm_copy(3).start()
            body(j, False, tops[...], parts[...], acts[...])
            return c
        lax.fori_loop(1, bodies - 1, body_step, 0)
        @pl.when(m >= 1)
        def _():
            if stages > 1:
                @pl.when(stage < last)
                def _():
                    send_copy(slot).wait_send()

                @pl.when(stage == last)
                def _():
                    keep_copy(0).wait()
            else:
                keep_copy(0).wait()

        if stages > 1:
            @pl.when(jnp.logical_and(stage < last, m >= 2))
            def _():
                pl.semaphore_wait(credit, 1)

        start(bodies - 1)
        w2_copy(lax.rem(m + bodies, 2), bodies).start()
        kn_copy(m).start()
        vn_copy(m).start()
        body(bodies - 1, True, tops[...], parts[...], acts[...])

        w2par = lax.rem(m + bodies, 2)
        w2_copy(w2par, 0).wait()

        w2_copy(1 - w2par, 0).start()

        sums = []
        cut = (pairs - 2) * pair
        for n in range(width // wide):
            cols = slice(n * wide, (n + 1) * wide)
            sums.append(mm(attn[:, 0:cut], w2s[w2par, 0:cut, cols]))
        for n in range(width // wide):
            cols = slice(n * wide, (n + 1) * wide)
            o = sums[n] + mm(attn[:, cut:width], w2s[w2par, cut:width, cols]) + acc[:, cols] + modp[3:4, cols]
            snd[:, cols] = (xs[slot, :, cols].astype(F32) + modp[2:3, cols] * o).astype(BF16)
        if stages > 1:
            @pl.when(stage < last)
            def _():
                for n in range(width // wide):
                    send_copy(slot, pl.ds(n * wide, wide)).start()

        if stages > 1:
            @pl.when(stage == last)
            def _():
                owner = m // per

                @pl.when(owner < last)
                def _():
                    give_copy(jnp.minimum(owner, last - 1), lax.rem(m, per)).start()

                @pl.when(owner == last)
                def _():
                    keep_copy(lax.rem(m, per)).start()

            @pl.when(jnp.logical_and(stage > 0, m + 2 < patches))
            def _():
                pl.semaphore_signal(credit, inc=1, device_id={'pp': jnp.maximum(stage - 1, 0)}, device_id_type=MESH)
        else:
            keep_copy(m).start()

        @pl.when(jnp.logical_and(stage == 0, m + 2 < patches))
        def _():
            x_copy(m + 2, slot).start()
        return carry

    lax.fori_loop(0, patches, patch_step, 0)

    kn_copy(0).wait()
    vn_copy(0).wait()
    w2_copy(patches % 2, 0).wait()
    if stages > 1:
        @pl.when(stage < last)
        def _():
            send_copy(0).wait_send()
            for place in range(per):
                give_copy(0, place).wait_recv()

        @pl.when(stage == last)
        def _():
            keep_copy(0).wait()
    else:
        keep_copy(0).wait()


def finish_kernel(parts, *refs):
    n = len(parts)
    srcs, dsts, bufs, rsem, wsem = refs[:n], refs[n:2 * n], refs[2 * n:3 * n], refs[3 * n], refs[3 * n + 1]
    reads = []
    writes = []
    for a in range(n):
        rows = srcs[a].shape[0] // parts[a]
        for p in range(parts[a]):
            here = pl.ds(p * rows, rows)
            i = len(reads)
            reads.append(pltpu.make_async_copy(srcs[a].at[here], bufs[a].at[here], rsem.at[i]))
            writes.append(pltpu.make_async_copy(bufs[a].at[here], dsts[a].at[here], wsem.at[i]))
    for r in reads:
        r.start()
    for r, w in zip(reads, writes):
        r.wait()
        w.start()
    for w in writes:
        w.wait()


def finish(arrays, parts):
    total = sum(parts)
    return pl.pallas_call(
        functools.partial(finish_kernel, parts),
        out_shape=[jax.ShapeDtypeStruct(a.shape, a.dtype) for a in arrays],
        in_specs=[pl.BlockSpec(memory_space=pltpu.HBM)] * len(arrays),
        out_specs=[pl.BlockSpec(memory_space=pltpu.HBM)] * len(arrays),
        scratch_shapes=[pltpu.VMEM(a.shape, a.dtype) for a in arrays] + [pltpu.SemaphoreType.DMA((total,))] * 2,
        compiler_params=pltpu.CompilerParams(vmem_limit_bytes=67043328),
        name="finish")(*[pltpu.with_memory_space_constraint(a, memory_space=pltpu.HBM) for a in arrays])


def rope_rows(head_dim):
    axis_zero = head_dim // 8
    axis_rest = (head_dim - axis_zero) // 2
    rows = []
    axes = []
    for dim in (axis_zero, axis_rest, head_dim - axis_zero - axis_rest):
        axes.append((len(rows), len(rows) + dim // 2))
        rows += [float(np.float32(1.0 / 10000.0 ** (i / dim))) for i in range(0, dim, 2)]
    return rows, axes


def make_stage(stages):
    def stage_program(x_in, cond_vec, pos_ids, w_mod, b_mod, w_one, b_one, qk_scale, w_two, b_two, k_prev, v_prev):
        batch, patches, tok, width = x_in.shape
        hd = qk_scale.shape[-1]
        mlp = w_two.shape[1] - width
        seq = patches * tok
        pair = 2 * hd
        pairs = width // pair
        mcol = mlp // pairs
        per = patches // stages
        hbm = functools.partial(pltpu.with_memory_space_constraint, memory_space=pltpu.HBM)
        dims = (stages, patches, tok, width, mlp, hd)
        out_patches = per
        x_out, k_new, v_new = pl.pallas_call(
            functools.partial(block_kernel, dims),
            out_shape=(jax.ShapeDtypeStruct((out_patches, tok, width), BF16),
                       jax.ShapeDtypeStruct((seq, width), BF16), jax.ShapeDtypeStruct((seq, width), BF16)),
            in_specs=[pl.BlockSpec(memory_space=pltpu.HBM)] * 6 + [pl.BlockSpec(memory_space=pltpu.VMEM)] * 6,
            out_specs=(pl.BlockSpec(memory_space=pltpu.HBM),) * 3,
            scratch_shapes=[
                pltpu.VMEM((width, 3 * width + mlp), BF16),
                pltpu.VMEM((2, 3 * mcol, width), BF16),
                pltpu.VMEM((seq, width), BF16),
                pltpu.VMEM((width, seq), BF16),
                pltpu.VMEM((12, 2 * tok, 2 * tok), F32),
                pltpu.VMEM((1, 2 * tok), F32),
                pltpu.VMEM((8, 2 * tok), F32),
                pltpu.VMEM((tok, mcol), BF16),
                pltpu.VMEM((pairs, 2 * pair, 2 * tok), BF16),
                pltpu.VMEM((tok, width), BF16),
                pltpu.VMEM((2, tok, width), BF16),
                pltpu.VMEM((tok, width), BF16),
                pltpu.VMEM((tok, width), F32),
                pltpu.VMEM((tok, width), BF16),
                pltpu.VMEM((tok, width), BF16),
                pltpu.VMEM((4, width), F32),
                pltpu.VMEM((1, 3 * width + mlp), F32),
                pltpu.VMEM((4, hd, tok), F32),
                pltpu.VMEM((hd // 2, tok), F32),
                pltpu.SemaphoreType.DMA((3,)),
                pltpu.SemaphoreType.DMA((pairs // 3,)),
                pltpu.SemaphoreType.DMA((2,)),
                pltpu.SemaphoreType.DMA,
                pltpu.SemaphoreType.DMA((4,)),
                pltpu.SemaphoreType.DMA((2,)),
                pltpu.SemaphoreType.DMA,
                pltpu.SemaphoreType.DMA((per,)),
                pltpu.SemaphoreType.DMA,
                pltpu.SemaphoreType.DMA,
                pltpu.SemaphoreType.DMA((3,)),
                pltpu.SemaphoreType.REGULAR,
            ],
            compiler_params=pltpu.CompilerParams(
                vmem_limit_bytes=67043328, **(dict(collective_id=0, has_side_effects=True) if stages > 1 else {})),
            name='blocks',
        )(hbm(x_in[0]), hbm(w_one[0]), hbm(w_two[0]), hbm(k_prev.reshape(seq, width)), hbm(v_prev.reshape(seq, width)),
          hbm(w_mod[0]), cond_vec, b_mod, b_one, b_two, pos_ids.transpose(2, 0, 1), qk_scale[0])
        if stages > 1:
            x_out, k_new, v_new = finish([x_out, k_new, v_new], (1, 2, 2))
        return x_out[None], k_new.reshape(k_prev.shape), v_new.reshape(v_prev.shape)
    return stage_program


def solution(mesh):
    stages = mesh.shape['pp']
    return jax.shard_map(
        make_stage(stages), mesh=mesh,
        in_specs=(P('dp'), P('dp'), P(), P('pp'), P('pp'), P('pp'), P('pp'), P('pp'), P('pp'), P('pp'), P('pp', 'dp'), P('pp', 'dp')),
        out_specs=(P('dp', 'pp'), P('pp', 'dp'), P('pp', 'dp')),
        check_vma=False)
```

```python
import functools
import math

import jax
import jax.numpy as jnp
import numpy as np
from jax import lax
from jax.experimental import pallas as pl
from jax.experimental.pallas import tpu as pltpu
from jax.sharding import PartitionSpec as P

MESH = pl.DeviceIdType.MESH
F32 = jnp.float32
BF16 = jnp.bfloat16
LOG2E = 1.4426950408889634


DOWNS = (0, 1, 4, 8, 9, 12, 16, 17, 20)
LASTS = (2, 4, 6, 10, 16, 17, 19, 21, 23)
UPS = (2, 3, 4, 5, 6, 7)


QKAT = 9
UPAT = 9
WAITAT = 9
EARLY = ((0, 0, 0, 1, 1, 1), (0, 2, 4))


def mm(a, b):
    return jnp.dot(a, b, preferred_element_type=F32)


def gelu(u):
    inner = u * (0.7978845608028654 + 0.035677408136300125 * (u * u))
    half = 0.5 * u
    return half + half * jnp.tanh(inner)


def block_kernel(dims, x_hbm, w1_hbm, w2_hbm, kp_hbm, vp_hbm, wmod_hbm, cond, bmod, b1_in, b2_in, pos, gains,
                 xo_hbm, kn_hbm, vn_hbm,
                 w1, w2s, kbuf, vt, sbufs, acts, qrhs, h, xs, snd, acc, attn, vst, gtab, freqs, tops, parts, modp, b1,
                 w1_sem, wm_sem, w2s_sem, kp_sem, vp_sem, x_sem, snd_sem, xo_sem, kn_sem, vn_sem, mod_sem, credit):
    stages, patches, tok, width, mlp, hd = dims
    seq = patches * tok
    pair = 2 * hd
    pairs = width // pair
    qkv = 3 * width
    mcol = mlp // pairs
    group = 3
    bodies = pairs // group
    span = group * mcol
    per = patches // stages
    expc = LOG2E / math.sqrt(hd)
    stage = lax.axis_index('pp') if stages > 1 else jnp.int32(0)
    last = stages - 1

    def w1_copy(j):
        cols = pl.ds(j * (qkv // 3), qkv // 3)
        return pltpu.make_async_copy(w1_hbm.at[:, cols], w1.at[:, cols], w1_sem.at[j])

    def wm_copy(j):
        if isinstance(j, int):
            lo = 0 if j == 0 else j * span + mcol
            cols = pl.ds(qkv + lo, min((j + 1) * span + mcol, mlp) - lo)
        else:
            cols = pl.ds(pl.multiple_of(qkv + j * span + mcol, mcol), span)
        return pltpu.make_async_copy(w1_hbm.at[:, cols], w1.at[:, cols], wm_sem.at[j])

    def w2_copy(par, j):
        row = j * span + width if j < bodies else 0
        return pltpu.make_async_copy(w2_hbm.at[pl.ds(row, span), :], w2s.at[par], w2s_sem.at[par])

    def w2_next(par, j):
        row = pl.multiple_of(j * span + width, mcol)
        return pltpu.make_async_copy(w2_hbm.at[pl.ds(row, span), :], w2s.at[par], w2s_sem.at[par])

    kp_copy = pltpu.make_async_copy(kp_hbm.at[pl.ds(tok, seq - tok), :], kbuf.at[pl.ds(tok, seq - tok), :], kp_sem)

    vrows = mcol
    vparts = seq // vrows

    def vp_part(p):
        return divmod(p * vrows, span)

    def vp_copy(p):
        par, row = vp_part(p)
        return pltpu.make_async_copy(vp_hbm.at[pl.ds(p * vrows, vrows), :], w2s.at[par, pl.ds(row, vrows), :], vp_sem.at[p])

    def x_copy(m, slot):
        return pltpu.make_async_copy(x_hbm.at[m], xs.at[slot], x_sem.at[slot])

    def mod_copy(c):
        cols = pl.ds(c * width, width)
        return pltpu.make_async_copy(wmod_hbm.at[:, cols], w1.at[:, pl.ds(qkv + c * width, width)], mod_sem.at[c])

    def kn_copy(m):
        rows = pl.ds(pl.multiple_of(m * tok, tok), tok)
        return pltpu.make_async_copy(kbuf.at[rows, :], kn_hbm.at[rows, :], kn_sem)

    def vn_copy(m):
        rows = pl.ds(pl.multiple_of(m * tok, tok), tok)
        return pltpu.make_async_copy(vst, vn_hbm.at[rows, :], vn_sem)

    def send_copy(slot, cols=pl.ds(0, width)):
        return pltpu.make_async_remote_copy(
            src_ref=snd.at[:, cols], dst_ref=xs.at[slot, :, cols], send_sem=snd_sem, recv_sem=x_sem.at[slot],
            device_id={'pp': jnp.minimum(stage + 1, last)}, device_id_type=MESH)

    def give_copy(owner, place):
        return pltpu.make_async_remote_copy(
            src_ref=snd, dst_ref=xo_hbm.at[place], send_sem=snd_sem, recv_sem=xo_sem.at[place],
            device_id={'pp': owner}, device_id_type=MESH)

    def keep_copy(place):
        return pltpu.make_async_copy(snd, xo_hbm.at[place], snd_sem)

    if stages > 1:
        barrier = pltpu.get_barrier_semaphore()

        def greet(d, c):
            pl.semaphore_signal(barrier, inc=1, device_id={'pp': lax.rem(stage + d, stages)}, device_id_type=MESH)
            return c
        lax.fori_loop(1, stages, greet, 0)

    @pl.when(stage == 0)
    def _():
        x_copy(0, 0).start()
        x_copy(1, 1).start()
    for c in range(3):
        mod_copy(c).start()
    for p in range(vparts):
        vp_copy(p).start()
    for j in range(3):
        w1_copy(j).start()
    kp_copy.start()

    qrhs[...] = jnp.zeros_like(qrhs)
    b1[...] = b1_in[...].astype(F32)

    freq_rows, axes = rope_rows(hd)
    row8 = lax.broadcasted_iota(jnp.int32, (8, tok), 0)
    for g in range(hd // 16):
        part = jnp.zeros((8, tok), F32)
        for r in range(8):
            part = jnp.where(row8 == r, freq_rows[8 * g + r], part)
        freqs[8 * g:8 * g + 8, :] = part
    odd_row = (lax.broadcasted_iota(jnp.int32, (hd, tok), 0) % 2) == 1

    def swap(v):
        v3 = v.reshape(hd // 8, 8, tok)
        return jnp.where(odd_row, pltpu.roll(v3, 1, 1).reshape(hd, tok), pltpu.roll(v3, 7, 1).reshape(hd, tok))

    def twice(v):
        return jnp.broadcast_to(v[:, None, :], (hd // 2, 2, tok)).reshape(hd, tok)

    for i in range(2):
        g = jnp.broadcast_to(gains[i:i + 1, :].astype(F32), (tok, hd)).T
        gtab[2 * i] = g
        gtab[2 * i + 1] = swap(g)
    modp[3:4, :] = b2_in[...].astype(F32)
    c32 = cond[...].astype(F32)
    act_c = (c32 * (1.0 / (1.0 + jnp.exp(-c32)))).astype(BF16)
    for c in range(3):
        mod_copy(c).wait()
        for n in range(width // mcol):
            lo = c * width + n * mcol
            v = mm(act_c, w1[:, qkv + lo:qkv + lo + mcol]) + bmod[:, lo:lo + mcol].astype(F32)
            modp[c:c + 1, n * mcol:(n + 1) * mcol] = v + 1.0 if c == 1 else v
    for p in range(vparts):
        vp_copy(p).wait()
        par, row = vp_part(p)

        def turn(d, c, p=p, par=par, row=row):
            ds = pl.ds(pl.multiple_of(d * pair, pair), pair)
            for t in range(vrows // tok):
                if p * vrows + t * tok >= tok:
                    vt[ds, pl.ds(p * vrows + t * tok, tok)] = w2s[par, pl.ds(row + t * tok, tok), ds].T
            return c
        lax.fori_loop(0, pairs, turn, 0, unroll=2)
    w2_copy(0, 0).start()
    wm_copy(0).start()
    wm_copy(1).start()
    for j in range(3):
        w1_copy(j).wait()

    if stages > 1:
        pl.semaphore_wait(barrier, stages - 1)

    def patch_step(m, carry):
        slot = lax.rem(m, 2)
        rows = pl.ds(pl.multiple_of(m * tok, tok), tok)
        x_copy(0, slot).wait()
        @pl.when(m >= 1)
        def _():
            vn_copy(0).wait()
            kn_copy(0).wait()

        w2_copy(lax.rem(m + 1, 2), 1).start()

        @pl.when(m == 0)
        def _():
            wm_copy(2).start()

        xv = xs[slot].astype(F32)
        cen = xv - jnp.mean(xv, axis=1, keepdims=True)
        nrm = cen * lax.rsqrt(jnp.mean(cen * cen, axis=1, keepdims=True) + 1e-6)
        h[...] = (nrm * modp[1:2, :] + modp[0:1, :]).astype(BF16)
        acc[...] = jnp.zeros_like(acc)

        angle = jnp.concatenate([freqs[lo:hi, :] * pos[axis, pl.ds(m, 1), :].astype(F32) for axis, (lo, hi) in enumerate(axes)], axis=0)
        cos_t = twice(jnp.cos(angle))
        sin_t = twice(jnp.sin(angle))
        sin_t = jnp.where(odd_row, sin_t, -sin_t)
        tab_q = (cos_t * gtab[0], sin_t * gtab[1])
        tab_k = (cos_t * gtab[2], sin_t * gtab[3])
        blk = 2 * pair

        def head_norm(raw, tabs):
            raw_t = raw.T.astype(F32)
            heads = []
            for r in range(2):
                part = raw_t[r * hd:(r + 1) * hd, :]
                ssq = jnp.sum(part * part, axis=0, keepdims=True)
                inv = lax.rsqrt(ssq * (1.0 / hd) + 1e-6)
                heads.append((part * tabs[0] + swap(part) * tabs[1]) * inv)
            return jnp.concatenate(heads, axis=0)

        wide = 2 * blk

        def proj(base, j):
            cols = slice(base + j * wide, base + (j + 1) * wide)
            return (mm(h[...], w1[:, cols]) + b1[:, cols]).astype(BF16)

        def put_q(raw, j):
            for t in range(4):
                n = 4 * j + t
                q32 = head_norm(raw[:, t * pair:(t + 1) * pair], tab_q).astype(BF16).astype(F32) * expc
                hi = q32.astype(BF16)
                lo = (q32 - hi.astype(F32)).astype(BF16)
                for r, qt in ((0, hi), (pair, lo)):
                    qrhs[n, r:r + hd, 0:tok] = qt[0:hd, :]
                    qrhs[n, r + hd:r + pair, tok:2 * tok] = qt[hd:pair, :]

        def put_k(raw, j):
            for t in range(4):
                n = 4 * j + t
                kbuf[rows, n * pair:(n + 1) * pair] = head_norm(raw[:, t * pair:(t + 1) * pair], tab_k).astype(BF16).T

        def put_v(raw, j):
            vst[:, j * wide:(j + 1) * wide] = raw
            vt[j * wide:(j + 1) * wide, rows] = raw.T

        ck = 2 * tok
        nck = seq // ck
        ring = 12
        lead = nck + 1

        def score(i, b, place):
            lanes = pl.ds(pl.multiple_of(i * pair, pair), pair)
            found = []
            for r in range(2):
                kc = kbuf[b * ck + r * tok:b * ck + (r + 1) * tok, lanes]
                v = mm(jnp.concatenate([kc, kc], axis=1), qrhs[i])
                sbufs[place, r * tok:(r + 1) * tok, :] = v
                found.append(jnp.max(v.reshape(tok // 8, 8, 2 * tok), axis=0))
            return jnp.maximum(found[0], found[1])

        def high(tops8):
            t8 = functools.reduce(jnp.maximum, tops8)
            return jnp.max(t8, axis=0, keepdims=True)

        held = None
        tops8 = []
        first = [(put, base, j) for j in range(width // wide) for put, base in ((put_q, 0), (put_k, width))]
        values = [(put_v, 2 * width, j) for j in range(width // wide)]
        order = first + values
        order = order[:QKAT] + ['score'] + order[QKAT:]
        order = order[:UPAT] + ['up'] + order[UPAT:]
        order = order[:WAITAT] + ['wait'] + order[WAITAT:]
        steps = group * nck
        kp = width // ck

        def plan(j, final):
            opening = isinstance(j, int) and j == 0
            places = {}
            for p in range(group):
                if not final or p < group - 1:
                    for k in range(kp):
                        places.setdefault(EARLY[0][k] if opening and p == 0 else nck * p + UPS[k], []).append(('up', p, k))
                for k in range(kp // 2):
                    if final:
                        at = LASTS[p * 3 + k]
                    else:
                        at = EARLY[1][k] if opening and p == 0 else DOWNS[p * 3 + k]
                    places.setdefault(at, []).append(('down', p, k))
            return places

        def up_piece(n, k):
            ks = slice(k * ck, (k + 1) * ck)
            return mm(h[:, ks], w1[ks, pl.ds(pl.multiple_of(qkv + n * mcol, mcol), mcol)])

        def activate(ups, n):
            up = (functools.reduce(jnp.add, ups) + b1[:, pl.ds(pl.multiple_of(qkv + n * mcol, mcol), mcol)]).astype(BF16)
            return gelu(up.astype(F32)).astype(BF16)

        def body(j, final, top, part, act0):
            par = lax.rem(m + j, 2)
            tops8 = [None] * nck + [part]
            places = plan(j, final)
            ups = []
            act = {0: act0}
            probs = None
            tots = []
            outs = []
            nexttop = None
            for t in range(steps + 1):
                u, b = divmod(t, nck)
                new = None
                if t < steps:
                    if b == 0 and u > 0:
                        top = nexttop
                    e = jnp.exp2(sbufs[t % ring] - top)
                    tots.append(jnp.sum(e.reshape(ck // 8, 8, 2 * tok), axis=0))
                    new = e.astype(BF16)
                    q = t + lead
                    if q < steps or not final:
                        tops8.append(score(group * j + q // nck, q % nck, q % ring))
                        if b == nck - 2:
                            nexttop = high(tops8[(u + 1) * nck:(u + 2) * nck])
                if t > 0:
                    pu, pb = divmod(t - 1, nck)
                    lanes = pl.ds(pl.multiple_of((group * j + pu) * pair, pair), pair)
                    outs.append(mm(vt[lanes, pb * ck:(pb + 1) * ck], probs))
                    if pb == nck - 1:
                        inv = 1.0 / jnp.sum(functools.reduce(jnp.add, tots[:nck]), axis=0, keepdims=True)
                        both = 0
                        for r in range(2):
                            out = functools.reduce(jnp.add, outs[r::2])
                            both = both + jnp.concatenate([out[0:hd, 0:tok] * inv[:, 0:tok], out[hd:pair, tok:2 * tok] * inv[:, tok:2 * tok]], axis=0)
                        attn[:, lanes] = both.astype(BF16).T
                        outs = []
                        tots = tots[nck:]
                probs = new
                for kind, p, k in places.get(t, ()):
                    if kind == 'up':
                        ups.append(up_piece(group * j + p + 1, k))
                        if k == kp - 1:
                            act[p + 1] = activate(ups, group * j + p + 1)
                            ups = []
                    else:
                        ks = slice(k * mcol, (k + 1) * mcol)
                        acc[:, ks] += mm(act[p], w2s[par, p * mcol:(p + 1) * mcol, ks])
            if not final:
                tops[...] = nexttop
                parts[...] = tops8[-1]
                acts[...] = act[group]

        for what in order:
            if what == 'wait':
                w2_copy(lax.rem(m, 2), 0).wait()

                @pl.when(m == 0)
                def _():
                    kp_copy.wait()
                    wm_copy(0).wait()
            elif what == 'score':
                tops8 = [score(0, b, b) for b in range(nck)]
                tops8.append(score(1, 0, nck))
            elif what == 'up':
                act0 = activate([up_piece(0, k) for k in range(kp)], 0)
            else:
                put, base, j = what
                raw = proj(base, j)
                if held is not None:
                    held[0](held[1], held[2])
                held = (put, raw, j)
        held[0](held[1], held[2])
        body(0, False, high(tops8[:nck]), tops8[nck], act0)

        def start(j):
            @pl.when(m == 0)
            def _():
                wm_copy(j).wait()
            w2_copy(lax.rem(m + j, 2), 0).wait()

        for j in range(1, bodies - 1):
            start(j)
            w2_next(lax.rem(m + j + 1, 2), j + 1).start()
            if j == 1:
                @pl.when(m == 0)
                def _():
                    wm_copy(3).start()
            body(j, False, tops[...], parts[...], acts[...])

        @pl.when(m >= 1)
        def _():
            if stages > 1:
                @pl.when(stage < last)
                def _():
                    send_copy(slot).wait_send()

                @pl.when(stage == last)
                def _():
                    keep_copy(0).wait()
            else:
                keep_copy(0).wait()

        if stages > 1:
            @pl.when(jnp.logical_and(stage < last, m >= 2))
            def _():
                pl.semaphore_wait(credit, 1)

        start(bodies - 1)
        w2_copy(lax.rem(m + bodies, 2), bodies).start()
        kn_copy(m).start()
        vn_copy(m).start()
        body(bodies - 1, True, tops[...], parts[...], acts[...])

        w2par = lax.rem(m + bodies, 2)
        w2_copy(w2par, 0).wait()

        w2_copy(1 - w2par, 0).start()

        sums = []
        cut = (pairs - 2) * pair
        for n in range(width // wide):
            cols = slice(n * wide, (n + 1) * wide)
            sums.append(mm(attn[:, 0:cut], w2s[w2par, 0:cut, cols]))
        for n in range(width // wide):
            cols = slice(n * wide, (n + 1) * wide)
            o = sums[n] + mm(attn[:, cut:width], w2s[w2par, cut:width, cols]) + acc[:, cols] + modp[3:4, cols]
            snd[:, cols] = (xs[slot, :, cols].astype(F32) + modp[2:3, cols] * o).astype(BF16)
        if stages > 1:
            @pl.when(stage < last)
            def _():
                for n in range(width // wide):
                    send_copy(slot, pl.ds(n * wide, wide)).start()

        if stages > 1:
            @pl.when(stage == last)
            def _():
                owner = m // per

                @pl.when(owner < last)
                def _():
                    give_copy(jnp.minimum(owner, last - 1), lax.rem(m, per)).start()

                @pl.when(owner == last)
                def _():
                    keep_copy(lax.rem(m, per)).start()

            @pl.when(jnp.logical_and(stage > 0, m + 2 < patches))
            def _():
                pl.semaphore_signal(credit, inc=1, device_id={'pp': jnp.maximum(stage - 1, 0)}, device_id_type=MESH)
        else:
            keep_copy(m).start()

        @pl.when(jnp.logical_and(stage == 0, m + 2 < patches))
        def _():
            x_copy(m + 2, slot).start()
        return carry

    lax.fori_loop(0, patches, patch_step, 0)

    kn_copy(0).wait()
    vn_copy(0).wait()
    w2_copy(patches % 2, 0).wait()
    if stages > 1:
        @pl.when(stage < last)
        def _():
            send_copy(0).wait_send()
            for place in range(per):
                give_copy(0, place).wait_recv()

        @pl.when(stage == last)
        def _():
            keep_copy(0).wait()
    else:
        keep_copy(0).wait()


def finish_kernel(parts, *refs):
    n = len(parts)
    srcs, dsts, bufs, rsem, wsem = refs[:n], refs[n:2 * n], refs[2 * n:3 * n], refs[3 * n], refs[3 * n + 1]
    reads = []
    writes = []
    for a in range(n):
        rows = srcs[a].shape[0] // parts[a]
        for p in range(parts[a]):
            here = pl.ds(p * rows, rows)
            i = len(reads)
            reads.append(pltpu.make_async_copy(srcs[a].at[here], bufs[a].at[here], rsem.at[i]))
            writes.append(pltpu.make_async_copy(bufs[a].at[here], dsts[a].at[here], wsem.at[i]))
    for r in reads:
        r.start()
    for r, w in zip(reads, writes):
        r.wait()
        w.start()
    for w in writes:
        w.wait()


def finish(arrays, parts):
    total = sum(parts)
    return pl.pallas_call(
        functools.partial(finish_kernel, parts),
        out_shape=[jax.ShapeDtypeStruct(a.shape, a.dtype) for a in arrays],
        in_specs=[pl.BlockSpec(memory_space=pltpu.HBM)] * len(arrays),
        out_specs=[pl.BlockSpec(memory_space=pltpu.HBM)] * len(arrays),
        scratch_shapes=[pltpu.VMEM(a.shape, a.dtype) for a in arrays] + [pltpu.SemaphoreType.DMA((total,))] * 2,
        compiler_params=pltpu.CompilerParams(vmem_limit_bytes=67043328),
        name="finish")(*[pltpu.with_memory_space_constraint(a, memory_space=pltpu.HBM) for a in arrays])


def rope_rows(head_dim):
    axis_zero = head_dim // 8
    axis_rest = (head_dim - axis_zero) // 2
    rows = []
    axes = []
    for dim in (axis_zero, axis_rest, head_dim - axis_zero - axis_rest):
        axes.append((len(rows), len(rows) + dim // 2))
        rows += [float(np.float32(1.0 / 10000.0 ** (i / dim))) for i in range(0, dim, 2)]
    return rows, axes


def make_stage(stages):
    def stage_program(x_in, cond_vec, pos_ids, w_mod, b_mod, w_one, b_one, qk_scale, w_two, b_two, k_prev, v_prev):
        batch, patches, tok, width = x_in.shape
        hd = qk_scale.shape[-1]
        mlp = w_two.shape[1] - width
        seq = patches * tok
        pair = 2 * hd
        pairs = width // pair
        mcol = mlp // pairs
        per = patches // stages
        hbm = functools.partial(pltpu.with_memory_space_constraint, memory_space=pltpu.HBM)
        dims = (stages, patches, tok, width, mlp, hd)
        out_patches = per
        x_out, k_new, v_new = pl.pallas_call(
            functools.partial(block_kernel, dims),
            out_shape=(jax.ShapeDtypeStruct((out_patches, tok, width), BF16),
                       jax.ShapeDtypeStruct((seq, width), BF16), jax.ShapeDtypeStruct((seq, width), BF16)),
            in_specs=[pl.BlockSpec(memory_space=pltpu.HBM)] * 6 + [pl.BlockSpec(memory_space=pltpu.VMEM)] * 6,
            out_specs=(pl.BlockSpec(memory_space=pltpu.HBM),) * 3,
            scratch_shapes=[
                pltpu.VMEM((width, 3 * width + mlp), BF16),
                pltpu.VMEM((2, 3 * mcol, width), BF16),
                pltpu.VMEM((seq, width), BF16),
                pltpu.VMEM((width, seq), BF16),
                pltpu.VMEM((12, 2 * tok, 2 * tok), F32),
                pltpu.VMEM((tok, mcol), BF16),
                pltpu.VMEM((pairs, 2 * pair, 2 * tok), BF16),
                pltpu.VMEM((tok, width), BF16),
                pltpu.VMEM((2, tok, width), BF16),
                pltpu.VMEM((tok, width), BF16),
                pltpu.VMEM((tok, width), F32),
                pltpu.VMEM((tok, width), BF16),
                pltpu.VMEM((tok, width), BF16),
                pltpu.VMEM((4, hd, tok), F32),
                pltpu.VMEM((hd // 2, tok), F32),
                pltpu.VMEM((1, 2 * tok), F32),
                pltpu.VMEM((8, 2 * tok), F32),
                pltpu.VMEM((4, width), F32),
                pltpu.VMEM((1, 3 * width + mlp), F32),
                pltpu.SemaphoreType.DMA((3,)),
                pltpu.SemaphoreType.DMA((pairs // 3,)),
                pltpu.SemaphoreType.DMA((2,)),
                pltpu.SemaphoreType.DMA,
                pltpu.SemaphoreType.DMA((4,)),
                pltpu.SemaphoreType.DMA((2,)),
                pltpu.SemaphoreType.DMA,
                pltpu.SemaphoreType.DMA((per,)),
                pltpu.SemaphoreType.DMA,
                pltpu.SemaphoreType.DMA,
                pltpu.SemaphoreType.DMA((3,)),
                pltpu.SemaphoreType.REGULAR,
            ],
            compiler_params=pltpu.CompilerParams(
                vmem_limit_bytes=67043328, **(dict(collective_id=0, has_side_effects=True) if stages > 1 else {})),
            name='blocks',
        )(hbm(x_in[0]), hbm(w_one[0]), hbm(w_two[0]), hbm(k_prev.reshape(seq, width)), hbm(v_prev.reshape(seq, width)),
          hbm(w_mod[0]), cond_vec, b_mod, b_one, b_two, pos_ids.transpose(2, 0, 1), qk_scale[0])
        if stages > 1:
            x_out, k_new, v_new = finish([x_out, k_new, v_new], (1, 2, 2))
        return x_out[None], k_new.reshape(k_prev.shape), v_new.reshape(v_prev.shape)
    return stage_program


def solution(mesh):
    stages = mesh.shape['pp']
    return jax.shard_map(
        make_stage(stages), mesh=mesh,
        in_specs=(P('dp'), P('dp'), P(), P('pp'), P('pp'), P('pp'), P('pp'), P('pp'), P('pp'), P('pp'), P('pp', 'dp'), P('pp', 'dp')),
        out_specs=(P('dp', 'pp'), P('pp', 'dp'), P('pp', 'dp')),
        check_vma=False)
```

```python
import functools
import math

import jax
import jax.numpy as jnp
import numpy as np
from jax import lax
from jax.experimental import pallas as pl
from jax.experimental.pallas import tpu as pltpu
from jax.sharding import PartitionSpec as P

MESH = pl.DeviceIdType.MESH
F32 = jnp.float32
BF16 = jnp.bfloat16
LOG2E = 1.4426950408889634


DOWNS = (0, 1, 4, 8, 9, 12, 16, 17, 20)
LASTS = (2, 4, 6, 10, 16, 17, 19, 21, 23)
UPS = (2, 3, 4, 5, 6, 7)


QKAT = 9
UPAT = 9
WAITAT = 9
EARLY = ((0, 0, 0, 1, 1, 1), (0, 2, 4))


def mm(a, b):
    return jnp.dot(a, b, preferred_element_type=F32)


def gelu(u):
    inner = u * (0.7978845608028654 + 0.035677408136300125 * (u * u))
    half = 0.5 * u
    return half + half * jnp.tanh(inner)


def block_kernel(dims, x_hbm, w1_hbm, w2_hbm, kp_hbm, vp_hbm, wmod_hbm, cond, bmod, b1_in, b2_in, pos, gains,
                 xo_hbm, kn_hbm, vn_hbm,
                 w1, w2s, kbuf, vt, sbufs, acts, qrhs, h, xs, snd, acc, attn, vst, gtab, freqs, tops, parts, modp, b1,
                 w1_sem, wm_sem, w2s_sem, kp_sem, vp_sem, x_sem, snd_sem, xo_sem, kn_sem, vn_sem, mod_sem, credit):
    stages, patches, tok, width, mlp, hd = dims
    seq = patches * tok
    pair = 2 * hd
    pairs = width // pair
    qkv = 3 * width
    mcol = mlp // pairs
    group = 3
    bodies = pairs // group
    span = group * mcol
    per = patches // stages
    expc = LOG2E / math.sqrt(hd)
    stage = lax.axis_index('pp') if stages > 1 else jnp.int32(0)
    last = stages - 1

    def w1_copy(j):
        cols = pl.ds(j * (qkv // 3), qkv // 3)
        return pltpu.make_async_copy(w1_hbm.at[:, cols], w1.at[:, cols], w1_sem.at[j])

    def wm_copy(j):
        if isinstance(j, int):
            lo = 0 if j == 0 else j * span + mcol
            cols = pl.ds(qkv + lo, min((j + 1) * span + mcol, mlp) - lo)
        else:
            cols = pl.ds(pl.multiple_of(qkv + j * span + mcol, mcol), span)
        return pltpu.make_async_copy(w1_hbm.at[:, cols], w1.at[:, cols], wm_sem.at[j])

    def w2_copy(par, j):
        row = j * span + width if j < bodies else 0
        return pltpu.make_async_copy(w2_hbm.at[pl.ds(row, span), :], w2s.at[par], w2s_sem.at[par])

    def w2_next(par, j):
        row = pl.multiple_of(j * span + width, mcol)
        return pltpu.make_async_copy(w2_hbm.at[pl.ds(row, span), :], w2s.at[par], w2s_sem.at[par])

    kp_copy = pltpu.make_async_copy(kp_hbm.at[pl.ds(tok, seq - tok), :], kbuf.at[pl.ds(tok, seq - tok), :], kp_sem)

    vrows = mcol
    vparts = seq // vrows

    def vp_part(p):
        return divmod(p * vrows, span)

    def vp_copy(p):
        par, row = vp_part(p)
        return pltpu.make_async_copy(vp_hbm.at[pl.ds(p * vrows, vrows), :], w2s.at[par, pl.ds(row, vrows), :], vp_sem.at[p])

    def x_copy(m, slot):
        return pltpu.make_async_copy(x_hbm.at[m], xs.at[slot], x_sem.at[slot])

    def mod_copy(c):
        cols = pl.ds(c * width, width)
        return pltpu.make_async_copy(wmod_hbm.at[:, cols], w1.at[:, pl.ds(qkv + c * width, width)], mod_sem.at[c])

    def kn_copy(m):
        rows = pl.ds(pl.multiple_of(m * tok, tok), tok)
        return pltpu.make_async_copy(kbuf.at[rows, :], kn_hbm.at[rows, :], kn_sem)

    def vn_copy(m):
        rows = pl.ds(pl.multiple_of(m * tok, tok), tok)
        return pltpu.make_async_copy(vst, vn_hbm.at[rows, :], vn_sem)

    def send_copy(slot, cols=pl.ds(0, width)):
        return pltpu.make_async_remote_copy(
            src_ref=snd.at[:, cols], dst_ref=xs.at[slot, :, cols], send_sem=snd_sem, recv_sem=x_sem.at[slot],
            device_id={'pp': jnp.minimum(stage + 1, last)}, device_id_type=MESH)

    def give_copy(owner, place):
        return pltpu.make_async_remote_copy(
            src_ref=snd, dst_ref=xo_hbm.at[place], send_sem=snd_sem, recv_sem=xo_sem.at[place],
            device_id={'pp': owner}, device_id_type=MESH)

    def keep_copy(place):
        return pltpu.make_async_copy(snd, xo_hbm.at[place], snd_sem)

    if stages > 1:
        barrier = pltpu.get_barrier_semaphore()

        def greet(d, c):
            pl.semaphore_signal(barrier, inc=1, device_id={'pp': lax.rem(stage + d, stages)}, device_id_type=MESH)
            return c
        lax.fori_loop(1, stages, greet, 0)

    @pl.when(stage == 0)
    def _():
        x_copy(0, 0).start()
        x_copy(1, 1).start()
    for c in range(3):
        mod_copy(c).start()
    for p in range(vparts):
        vp_copy(p).start()
    for j in range(3):
        w1_copy(j).start()
    kp_copy.start()

    qrhs[...] = jnp.zeros_like(qrhs)
    b1[...] = b1_in[...].astype(F32)

    freq_rows, axes = rope_rows(hd)
    row8 = lax.broadcasted_iota(jnp.int32, (8, tok), 0)
    for g in range(hd // 16):
        part = jnp.zeros((8, tok), F32)
        for r in range(8):
            part = jnp.where(row8 == r, freq_rows[8 * g + r], part)
        freqs[8 * g:8 * g + 8, :] = part
    odd_row = (lax.broadcasted_iota(jnp.int32, (hd, tok), 0) % 2) == 1

    def swap(v):
        v3 = v.reshape(hd // 8, 8, tok)
        return jnp.where(odd_row, pltpu.roll(v3, 1, 1).reshape(hd, tok), pltpu.roll(v3, 7, 1).reshape(hd, tok))

    def twice(v):
        return jnp.broadcast_to(v[:, None, :], (hd // 2, 2, tok)).reshape(hd, tok)

    for i in range(2):
        g = jnp.broadcast_to(gains[i:i + 1, :].astype(F32), (tok, hd)).T
        gtab[2 * i] = g
        gtab[2 * i + 1] = swap(g)
    modp[3:4, :] = b2_in[...].astype(F32)
    c32 = cond[...].astype(F32)
    act_c = (c32 * (1.0 / (1.0 + jnp.exp(-c32)))).astype(BF16)
    for c in range(3):
        mod_copy(c).wait()
        for n in range(width // mcol):
            lo = c * width + n * mcol
            v = mm(act_c, w1[:, qkv + lo:qkv + lo + mcol]) + bmod[:, lo:lo + mcol].astype(F32)
            modp[c:c + 1, n * mcol:(n + 1) * mcol] = v + 1.0 if c == 1 else v
    for p in range(vparts):
        vp_copy(p).wait()
        par, row = vp_part(p)

        def turn(d, c, p=p, par=par, row=row):
            ds = pl.ds(pl.multiple_of(d * pair, pair), pair)
            for t in range(vrows // tok):
                if p * vrows + t * tok >= tok:
                    vt[ds, pl.ds(p * vrows + t * tok, tok)] = w2s[par, pl.ds(row + t * tok, tok), ds].T
            return c
        lax.fori_loop(0, pairs, turn, 0, unroll=2)
    w2_copy(0, 0).start()
    wm_copy(0).start()
    wm_copy(1).start()
    for j in range(3):
        w1_copy(j).wait()

    if stages > 1:
        pl.semaphore_wait(barrier, stages - 1)

    def patch_step(m, carry):
        slot = lax.rem(m, 2)
        rows = pl.ds(pl.multiple_of(m * tok, tok), tok)
        x_copy(0, slot).wait()
        @pl.when(m >= 1)
        def _():
            vn_copy(0).wait()
            kn_copy(0).wait()

        w2_copy(lax.rem(m + 1, 2), 1).start()

        @pl.when(m == 0)
        def _():
            wm_copy(2).start()

        xv = xs[slot].astype(F32)
        cen = xv - jnp.mean(xv, axis=1, keepdims=True)
        nrm = cen * lax.rsqrt(jnp.mean(cen * cen, axis=1, keepdims=True) + 1e-6)
        h[...] = (nrm * modp[1:2, :] + modp[0:1, :]).astype(BF16)

        angle = jnp.concatenate([freqs[lo:hi, :] * pos[axis, pl.ds(m, 1), :].astype(F32) for axis, (lo, hi) in enumerate(axes)], axis=0)
        cos_t = twice(jnp.cos(angle))
        sin_t = twice(jnp.sin(angle))
        sin_t = jnp.where(odd_row, sin_t, -sin_t)
        tab_q = (cos_t * gtab[0], sin_t * gtab[1])
        tab_k = (cos_t * gtab[2], sin_t * gtab[3])
        blk = 2 * pair

        def head_norm(raw, tabs):
            raw_t = raw.T.astype(F32)
            heads = []
            for r in range(2):
                part = raw_t[r * hd:(r + 1) * hd, :]
                ssq = jnp.sum(part * part, axis=0, keepdims=True)
                inv = lax.rsqrt(ssq * (1.0 / hd) + 1e-6)
                heads.append((part * tabs[0] + swap(part) * tabs[1]) * inv)
            return jnp.concatenate(heads, axis=0)

        wide = 2 * blk

        def proj(base, j):
            cols = slice(base + j * wide, base + (j + 1) * wide)
            return (mm(h[...], w1[:, cols]) + b1[:, cols]).astype(BF16)

        def put_q(raw, j):
            for t in range(4):
                n = 4 * j + t
                q32 = head_norm(raw[:, t * pair:(t + 1) * pair], tab_q).astype(BF16).astype(F32) * expc
                hi = q32.astype(BF16)
                lo = (q32 - hi.astype(F32)).astype(BF16)
                for r, qt in ((0, hi), (pair, lo)):
                    qrhs[n, r:r + hd, 0:tok] = qt[0:hd, :]
                    qrhs[n, r + hd:r + pair, tok:2 * tok] = qt[hd:pair, :]

        def put_k(raw, j):
            for t in range(4):
                n = 4 * j + t
                kbuf[rows, n * pair:(n + 1) * pair] = head_norm(raw[:, t * pair:(t + 1) * pair], tab_k).astype(BF16).T

        def put_v(raw, j):
            vst[:, j * wide:(j + 1) * wide] = raw
            vt[j * wide:(j + 1) * wide, rows] = raw.T

        ck = 2 * tok
        nck = seq // ck
        ring = 12
        lead = nck + 1

        def score(i, b, place):
            lanes = pl.ds(pl.multiple_of(i * pair, pair), pair)
            found = []
            for r in range(2):
                kc = kbuf[b * ck + r * tok:b * ck + (r + 1) * tok, lanes]
                v = mm(jnp.concatenate([kc, kc], axis=1), qrhs[i])
                sbufs[place, r * tok:(r + 1) * tok, :] = v
                found.append(jnp.max(v.reshape(tok // 8, 8, 2 * tok), axis=0))
            return jnp.maximum(found[0], found[1])

        def high(tops8):
            t8 = functools.reduce(jnp.maximum, tops8)
            return jnp.max(t8, axis=0, keepdims=True)

        held = None
        tops8 = []
        first = [(put, base, j) for j in range(width // wide) for put, base in ((put_q, 0), (put_k, width))]
        values = [(put_v, 2 * width, j) for j in range(width // wide)]
        order = first + values
        order = order[:QKAT] + ['score'] + order[QKAT:]
        order = order[:UPAT] + ['up'] + order[UPAT:]
        order = order[:WAITAT] + ['wait'] + order[WAITAT:]
        steps = group * nck
        kp = width // ck

        def plan(j, final):
            opening = isinstance(j, int) and j == 0
            places = {}
            for p in range(group):
                if not final or p < group - 1:
                    for k in range(kp):
                        places.setdefault(EARLY[0][k] if opening and p == 0 else nck * p + UPS[k], []).append(('up', p, k))
                for k in range(kp // 2):
                    if final:
                        at = LASTS[p * 3 + k]
                    else:
                        at = EARLY[1][k] if opening and p == 0 else DOWNS[p * 3 + k]
                    places.setdefault(at, []).append(('down', p, k))
            return places

        def up_piece(n, k):
            ks = slice(k * ck, (k + 1) * ck)
            return mm(h[:, ks], w1[ks, pl.ds(pl.multiple_of(qkv + n * mcol, mcol), mcol)])

        def activate(ups, n):
            up = (functools.reduce(jnp.add, ups) + b1[:, pl.ds(pl.multiple_of(qkv + n * mcol, mcol), mcol)]).astype(BF16)
            return gelu(up.astype(F32)).astype(BF16)

        def body(j, final, top, part, act0):
            par = lax.rem(m + j, 2)
            tops8 = [None] * nck + [part]
            places = plan(j, final)
            ups = []
            act = {0: act0}
            probs = None
            tots = []
            outs = []
            nexttop = None
            for t in range(steps + 1):
                u, b = divmod(t, nck)
                new = None
                if t < steps:
                    if b == 0 and u > 0:
                        top = nexttop
                    e = jnp.exp2(sbufs[t % ring] - top)
                    tots.append(jnp.sum(e.reshape(ck // 8, 8, 2 * tok), axis=0))
                    new = e.astype(BF16)
                    q = t + lead
                    if q < steps or not final:
                        tops8.append(score(group * j + q // nck, q % nck, q % ring))
                        if b == nck - 2:
                            nexttop = high(tops8[(u + 1) * nck:(u + 2) * nck])
                if t > 0:
                    pu, pb = divmod(t - 1, nck)
                    lanes = pl.ds(pl.multiple_of((group * j + pu) * pair, pair), pair)
                    outs.append(mm(vt[lanes, pb * ck:(pb + 1) * ck], probs))
                    if pb == nck - 1:
                        inv = 1.0 / jnp.sum(functools.reduce(jnp.add, tots[:nck]), axis=0, keepdims=True)
                        both = 0
                        for r in range(2):
                            out = functools.reduce(jnp.add, outs[r::2])
                            both = both + jnp.concatenate([out[0:hd, 0:tok] * inv[:, 0:tok], out[hd:pair, tok:2 * tok] * inv[:, tok:2 * tok]], axis=0)
                        attn[:, lanes] = both.astype(BF16).T
                        outs = []
                        tots = tots[nck:]
                probs = new
                for kind, p, k in places.get(t, ()):
                    if kind == 'up':
                        ups.append(up_piece(group * j + p + 1, k))
                        if k == kp - 1:
                            act[p + 1] = activate(ups, group * j + p + 1)
                            ups = []
                    else:
                        ks = slice(k * mcol, (k + 1) * mcol)
                        v = mm(act[p], w2s[par, p * mcol:(p + 1) * mcol, ks])
                        acc[:, ks] = v if j == 0 and p == 0 else acc[:, ks] + v
            if not final:
                tops[...] = nexttop
                parts[...] = tops8[-1]
                acts[...] = act[group]

        for what in order:
            if what == 'wait':
                w2_copy(lax.rem(m, 2), 0).wait()

                @pl.when(m == 0)
                def _():
                    kp_copy.wait()
                    wm_copy(0).wait()
            elif what == 'score':
                tops8 = [score(0, b, b) for b in range(nck)]
                tops8.append(score(1, 0, nck))
            elif what == 'up':
                act0 = activate([up_piece(0, k) for k in range(kp)], 0)
            else:
                put, base, j = what
                raw = proj(base, j)
                if held is not None:
                    held[0](held[1], held[2])
                held = (put, raw, j)
        held[0](held[1], held[2])
        body(0, False, high(tops8[:nck]), tops8[nck], act0)

        def start(j):
            @pl.when(m == 0)
            def _():
                wm_copy(j).wait()
            w2_copy(lax.rem(m + j, 2), 0).wait()

        for j in range(1, bodies - 1):
            start(j)
            w2_next(lax.rem(m + j + 1, 2), j + 1).start()
            if j == 1:
                @pl.when(m == 0)
                def _():
                    wm_copy(3).start()
            body(j, False, tops[...], parts[...], acts[...])

        @pl.when(m >= 1)
        def _():
            if stages > 1:
                @pl.when(stage < last)
                def _():
                    send_copy(slot).wait_send()

                @pl.when(stage == last)
                def _():
                    keep_copy(0).wait()
            else:
                keep_copy(0).wait()

        if stages > 1:
            @pl.when(jnp.logical_and(stage < last, m >= 2))
            def _():
                pl.semaphore_wait(credit, 1)

        start(bodies - 1)
        w2_copy(lax.rem(m + bodies, 2), bodies).start()
        kn_copy(m).start()
        vn_copy(m).start()
        body(bodies - 1, True, tops[...], parts[...], acts[...])

        w2par = lax.rem(m + bodies, 2)
        w2_copy(w2par, 0).wait()

        w2_copy(1 - w2par, 0).start()

        sums = []
        cut = (pairs - 2) * pair
        for n in range(width // wide):
            cols = slice(n * wide, (n + 1) * wide)
            sums.append(mm(attn[:, 0:cut], w2s[w2par, 0:cut, cols]))
        for n in range(width // wide):
            cols = slice(n * wide, (n + 1) * wide)
            o = sums[n] + mm(attn[:, cut:width], w2s[w2par, cut:width, cols]) + acc[:, cols] + modp[3:4, cols]
            snd[:, cols] = (xs[slot, :, cols].astype(F32) + modp[2:3, cols] * o).astype(BF16)
        if stages > 1:
            @pl.when(stage < last)
            def _():
                for n in range(width // wide):
                    send_copy(slot, pl.ds(n * wide, wide)).start()

        if stages > 1:
            @pl.when(stage == last)
            def _():
                owner = m // per

                @pl.when(owner < last)
                def _():
                    give_copy(jnp.minimum(owner, last - 1), lax.rem(m, per)).start()

                @pl.when(owner == last)
                def _():
                    keep_copy(lax.rem(m, per)).start()

            @pl.when(jnp.logical_and(stage > 0, m + 2 < patches))
            def _():
                pl.semaphore_signal(credit, inc=1, device_id={'pp': jnp.maximum(stage - 1, 0)}, device_id_type=MESH)
        else:
            keep_copy(m).start()

        @pl.when(jnp.logical_and(stage == 0, m + 2 < patches))
        def _():
            x_copy(m + 2, slot).start()
        return carry

    lax.fori_loop(0, patches, patch_step, 0)

    kn_copy(0).wait()
    vn_copy(0).wait()
    w2_copy(patches % 2, 0).wait()
    if stages > 1:
        @pl.when(stage < last)
        def _():
            send_copy(0).wait_send()
            for place in range(per):
                give_copy(0, place).wait_recv()

        @pl.when(stage == last)
        def _():
            keep_copy(0).wait()
    else:
        keep_copy(0).wait()


def finish_kernel(parts, *refs):
    n = len(parts)
    srcs, dsts, bufs, rsem, wsem = refs[:n], refs[n:2 * n], refs[2 * n:3 * n], refs[3 * n], refs[3 * n + 1]
    reads = []
    writes = []
    for a in range(n):
        rows = srcs[a].shape[0] // parts[a]
        for p in range(parts[a]):
            here = pl.ds(p * rows, rows)
            i = len(reads)
            reads.append(pltpu.make_async_copy(srcs[a].at[here], bufs[a].at[here], rsem.at[i]))
            writes.append(pltpu.make_async_copy(bufs[a].at[here], dsts[a].at[here], wsem.at[i]))
    for r in reads:
        r.start()
    for r, w in zip(reads, writes):
        r.wait()
        w.start()
    for w in writes:
        w.wait()


def finish(arrays, parts):
    total = sum(parts)
    return pl.pallas_call(
        functools.partial(finish_kernel, parts),
        out_shape=[jax.ShapeDtypeStruct(a.shape, a.dtype) for a in arrays],
        in_specs=[pl.BlockSpec(memory_space=pltpu.HBM)] * len(arrays),
        out_specs=[pl.BlockSpec(memory_space=pltpu.HBM)] * len(arrays),
        scratch_shapes=[pltpu.VMEM(a.shape, a.dtype) for a in arrays] + [pltpu.SemaphoreType.DMA((total,))] * 2,
        compiler_params=pltpu.CompilerParams(vmem_limit_bytes=67043328),
        name="finish")(*[pltpu.with_memory_space_constraint(a, memory_space=pltpu.HBM) for a in arrays])


def rope_rows(head_dim):
    axis_zero = head_dim // 8
    axis_rest = (head_dim - axis_zero) // 2
    rows = []
    axes = []
    for dim in (axis_zero, axis_rest, head_dim - axis_zero - axis_rest):
        axes.append((len(rows), len(rows) + dim // 2))
        rows += [float(np.float32(1.0 / 10000.0 ** (i / dim))) for i in range(0, dim, 2)]
    return rows, axes


def make_stage(stages):
    def stage_program(x_in, cond_vec, pos_ids, w_mod, b_mod, w_one, b_one, qk_scale, w_two, b_two, k_prev, v_prev):
        batch, patches, tok, width = x_in.shape
        hd = qk_scale.shape[-1]
        mlp = w_two.shape[1] - width
        seq = patches * tok
        pair = 2 * hd
        pairs = width // pair
        mcol = mlp // pairs
        per = patches // stages
        hbm = functools.partial(pltpu.with_memory_space_constraint, memory_space=pltpu.HBM)
        dims = (stages, patches, tok, width, mlp, hd)
        out_patches = per
        x_out, k_new, v_new = pl.pallas_call(
            functools.partial(block_kernel, dims),
            out_shape=(jax.ShapeDtypeStruct((out_patches, tok, width), BF16),
                       jax.ShapeDtypeStruct((seq, width), BF16), jax.ShapeDtypeStruct((seq, width), BF16)),
            in_specs=[pl.BlockSpec(memory_space=pltpu.HBM)] * 6 + [pl.BlockSpec(memory_space=pltpu.VMEM)] * 6,
            out_specs=(pl.BlockSpec(memory_space=pltpu.HBM),) * 3,
            scratch_shapes=[
                pltpu.VMEM((width, 3 * width + mlp), BF16),
                pltpu.VMEM((2, 3 * mcol, width), BF16),
                pltpu.VMEM((seq, width), BF16),
                pltpu.VMEM((width, seq), BF16),
                pltpu.VMEM((12, 2 * tok, 2 * tok), F32),
                pltpu.VMEM((tok, mcol), BF16),
                pltpu.VMEM((pairs, 2 * pair, 2 * tok), BF16),
                pltpu.VMEM((tok, width), BF16),
                pltpu.VMEM((2, tok, width), BF16),
                pltpu.VMEM((tok, width), BF16),
                pltpu.VMEM((tok, width), F32),
                pltpu.VMEM((tok, width), BF16),
                pltpu.VMEM((tok, width), BF16),
                pltpu.VMEM((4, hd, tok), F32),
                pltpu.VMEM((hd // 2, tok), F32),
                pltpu.VMEM((1, 2 * tok), F32),
                pltpu.VMEM((8, 2 * tok), F32),
                pltpu.VMEM((4, width), F32),
                pltpu.VMEM((1, 3 * width + mlp), F32),
                pltpu.SemaphoreType.DMA((3,)),
                pltpu.SemaphoreType.DMA((pairs // 3,)),
                pltpu.SemaphoreType.DMA((2,)),
                pltpu.SemaphoreType.DMA,
                pltpu.SemaphoreType.DMA((4,)),
                pltpu.SemaphoreType.DMA((2,)),
                pltpu.SemaphoreType.DMA,
                pltpu.SemaphoreType.DMA((per,)),
                pltpu.SemaphoreType.DMA,
                pltpu.SemaphoreType.DMA,
                pltpu.SemaphoreType.DMA((3,)),
                pltpu.SemaphoreType.REGULAR,
            ],
            compiler_params=pltpu.CompilerParams(
                vmem_limit_bytes=67043328, **(dict(collective_id=0, has_side_effects=True) if stages > 1 else {})),
            name='blocks',
        )(hbm(x_in[0]), hbm(w_one[0]), hbm(w_two[0]), hbm(k_prev.reshape(seq, width)), hbm(v_prev.reshape(seq, width)),
          hbm(w_mod[0]), cond_vec, b_mod, b_one, b_two, pos_ids.transpose(2, 0, 1), qk_scale[0])
        if stages > 1:
            x_out, k_new, v_new = finish([x_out, k_new, v_new], (1, 2, 2))
        return x_out[None], k_new.reshape(k_prev.shape), v_new.reshape(v_prev.shape)
    return stage_program


def solution(mesh):
    stages = mesh.shape['pp']
    return jax.shard_map(
        make_stage(stages), mesh=mesh,
        in_specs=(P('dp'), P('dp'), P(), P('pp'), P('pp'), P('pp'), P('pp'), P('pp'), P('pp'), P('pp'), P('pp', 'dp'), P('pp', 'dp')),
        out_specs=(P('dp', 'pp'), P('pp', 'dp'), P('pp', 'dp')),
        check_vma=False)
```
